32 devices in a mesh: grp: 4 (over y, x), dom: 8 (over z, core).
Axes of the slice: x: 2, y: 2, z: 4, core: 2. Of those that a mesh axis runs over, the one named last changes fastest.
Arguments:
- forcing: float32 [3, 2048, 512], P(None, 'dom'), may hold values from -144 to 144
- viscosity: float32 [2048], P('dom'), may hold values from 0.3 to 3
- mass_coef: float32 [2048], P('dom'), may hold values from 8 to 80
- element_order: int32 [8, 256], P('dom'), may hold values from 0 to 255, each once within a row
- owner: int32 [8, 256], P('dom'), may hold values from -1 to 7, as said below
Outputs:
- fields: float32 [4, 2048, 512], P('grp', 'dom')
The draws below stay inside these ranges and needn't reach their ends.
Inputs may be any that keep to these rules, and one draw needn't show every extreme that they name: `element_order`: row d gives each element slot of partition d its cell in the partition's brick of 8 x 8 x 4 elements, every cell once. -1 marks an element that is not analysed; at most 32 elements of one partition have the same owner, and some owner gets exactly 32 from every partition.
All inputs are finite; a program needn't handle non-finite values.
Results may differ from the reference program's by a relative error of at most 0.00037.
Values may be sent and summed in bfloat16 or wider, within the bound.
No kernel may reach another device: no remote copies, remote signals or barrier semaphores. Data moves between devices by JAX's collectives and lax.ppermute only.
A program may use at most 64 MiB of HBM per device.

```python
import math
import jax
import jax.numpy as jnp
import numpy as np
from jax import lax

NP = 8
NODES = 512
BX = 8
BY = 8
BZ = 4
ITERS = 4
SWEEPS = 4
E_DEV = 256
ELEMS = 2048
CAP = 32
N_DOM = 8


def draw_owner(key, part):
    levels = jax.random.randint(jax.random.fold_in(key, 11), (N_DOM,), 1, 5)
    full_owner = jax.random.randint(jax.random.fold_in(key, 12), (), 0, N_DOM)
    levels = jnp.where(jnp.arange(N_DOM) == full_owner, 8, levels)
    tickets = jnp.arange(E_DEV) // CAP

    def one_partition(part_key):
        ordering = jax.random.permutation(part_key, E_DEV)
        keeping = jax.random.randint(jax.random.fold_in(part_key, 1), (E_DEV,), 0, 8) < levels[tickets]
        kept_owner = jnp.where(keeping, tickets, -1)
        return kept_owner[ordering]
    part_keys = jax.random.split(jax.random.fold_in(key, 13), N_DOM)
    return jax.vmap(one_partition)(part_keys).astype(jnp.int32)


def block_levels(stream_key, dims, pieces, low, top_value):
    def one(axis_at, shards_of):
        steps = jax.random.uniform(jax.random.fold_in(jax.random.fold_in(stream_key, 6), axis_at), (shards_of,), jnp.float32, low / len(pieces), top_value / len(pieces))
        return jnp.repeat(jnp.exp(steps), dims[axis_at] // shards_of).reshape((-1,) + (1,) * (len(dims) - axis_at - 1))

    factor_of = one(*pieces[0])
    for cut in pieces[1:]:
        factor_of = factor_of * one(*cut)
    return factor_of


def scatter_about(stream_key, shape, scale, limit, cuts=(), kind=jnp.bfloat16):
    values = jax.random.normal(stream_key, shape, jnp.float32) * scale
    if len(cuts) > 0:
        values = block_levels(stream_key, shape, cuts, -0.22, 0.18) * values
    return jnp.clip(values, min=-limit, max=limit).astype(kind)


def setup_inputs(seed: int = 0) -> dict:
    arg_keys = jax.random.split(jax.random.key(seed), 6)
    forcing = scatter_about(arg_keys[0], (3, ELEMS, NODES), 24.0, 144.0, ((1, 8),), jnp.float32)
    viscosity = jnp.clip(jnp.exp(math.log(3.0) - 2.3025851 * jax.random.uniform(arg_keys[1], (ELEMS,), jnp.float32) ** block_levels(arg_keys[1], (ELEMS,), ((0, 8),), -0.2, 0.2)), 0.3, 3.0)
    mass_coef = jnp.clip(jnp.exp(math.log(80.0) - 2.3025851 * jax.random.uniform(arg_keys[2], (ELEMS,), jnp.float32) ** block_levels(arg_keys[2], (ELEMS,), ((0, 8),), -0.2, 0.2)), 8.0, 80.0)
    element_order = jax.vmap(lambda own: jax.random.permutation(own, E_DEV))(jax.random.split(arg_keys[3], N_DOM)).reshape((N_DOM, E_DEV)).astype(jnp.int32)
    owner = draw_owner(jax.random.fold_in(arg_keys[5], 71), 0)
    return dict(forcing=forcing, viscosity=viscosity, mass_coef=mass_coef, element_order=element_order, owner=owner)


def legendre_values(points, node_count):
    legendre = np.zeros((points.shape[0], node_count))
    legendre[:, 0] = 1.0
    legendre[:, 1] = points
    for poly_order in range(2, node_count):
        legendre[:, poly_order] = ((2 * poly_order - 1) * points * legendre[:, poly_order - 1] - (poly_order - 1) * legendre[:, poly_order - 2]) / poly_order
    return legendre


def lobatto_table(node_count):
    degree = node_count - 1
    points = np.cos(np.pi * np.arange(node_count) / degree)
    for attempt in range(60):
        legendre = legendre_values(points, node_count)
        points = points - (points * legendre[:, degree] - legendre[:, degree - 1]) / (node_count * legendre[:, degree])
    points = points[::-1].copy()
    end_values = legendre_values(points, node_count)[:, degree]
    weights = 2.0 / (degree * node_count * end_values * end_values)
    spacing = points[:, None] - points[None, :] + np.eye(node_count)
    diff_matrix = end_values[:, None] / end_values[None, :] / spacing
    diff_matrix = diff_matrix * (1.0 - np.eye(node_count))
    diff_matrix[0, 0] = -degree * node_count / 4.0
    diff_matrix[-1, -1] = degree * node_count / 4.0
    return weights, diff_matrix


def operator_tables(node_count):
    weights, diff_matrix = lobatto_table(node_count)
    identity = np.eye(node_count)
    weight_cube = (weights[:, None, None] * weights[None, :, None] * weights[None, None, :]).reshape(-1)
    directional = [np.kron(identity, np.kron(identity, diff_matrix)), np.kron(identity, np.kron(diff_matrix, identity)), np.kron(diff_matrix, np.kron(identity, identity))]
    stiffness = np.zeros((node_count ** 3, node_count ** 3))
    for direction_matrix in directional:
        stiffness = stiffness + direction_matrix.T @ (weight_cube[:, None] * direction_matrix)
    return diff_matrix, weight_cube, stiffness


def lambda_two(jacobian):
    strain = [[0.5 * (jacobian[first_index][second_index] + jacobian[second_index][first_index]) for second_index in range(3)] for first_index in range(3)]
    rotation_rate = [[0.5 * (jacobian[first_index][second_index] - jacobian[second_index][first_index]) for second_index in range(3)] for first_index in range(3)]
    matrix = [[None, None, None], [None, None, None], [None, None, None]]
    for first_index in range(3):
        for second_index in range(first_index, 3):
            entry_value = strain[first_index][0] * strain[0][second_index] + rotation_rate[first_index][0] * rotation_rate[0][second_index]
            for middle_index in (1, 2):
                entry_value = entry_value + strain[first_index][middle_index] * strain[middle_index][second_index] + rotation_rate[first_index][middle_index] * rotation_rate[middle_index][second_index]
            matrix[first_index][second_index] = entry_value
            matrix[second_index][first_index] = entry_value
    for sweep_index in range(SWEEPS):
        for first_index, second_index, third_index in ((0, 1, 2), (0, 2, 1), (1, 2, 0)):
            pivot_entry = matrix[first_index][second_index]
            first_diag = matrix[first_index][first_index]
            second_diag = matrix[second_index][second_index]
            rotation = 0.5 * jnp.arctan2(2.0 * pivot_entry, first_diag - second_diag)
            cosine = jnp.cos(rotation)
            sine_part = jnp.sin(rotation)
            new_first_diag = cosine * cosine * first_diag + 2.0 * cosine * sine_part * pivot_entry + sine_part * sine_part * second_diag
            new_second_diag = sine_part * sine_part * first_diag - 2.0 * cosine * sine_part * pivot_entry + cosine * cosine * second_diag
            side_first = matrix[third_index][first_index]
            side_second = matrix[third_index][second_index]
            new_side_first = cosine * side_first + sine_part * side_second
            new_side_second = cosine * side_second - sine_part * side_first
            matrix[first_index][first_index] = new_first_diag
            matrix[second_index][second_index] = new_second_diag
            matrix[first_index][second_index] = jnp.zeros_like(pivot_entry)
            matrix[second_index][first_index] = jnp.zeros_like(pivot_entry)
            matrix[third_index][first_index] = new_side_first
            matrix[first_index][third_index] = new_side_first
            matrix[third_index][second_index] = new_side_second
            matrix[second_index][third_index] = new_side_second
    diagonal = [matrix[0][0], matrix[1][1], matrix[2][2]]
    trace_sum = diagonal[0] + diagonal[1] + diagonal[2]
    largest = jnp.maximum(jnp.maximum(diagonal[0], diagonal[1]), diagonal[2])
    smallest = jnp.minimum(jnp.minimum(diagonal[0], diagonal[1]), diagonal[2])
    return trace_sum - largest - smallest


def reference(forcing, viscosity, mass_coef, element_order, owner):
    highest = lax.Precision.HIGHEST
    diff_np, weight_np, stiff_np = operator_tables(NP)
    diff_matrix = jnp.asarray(diff_np, jnp.float32)
    weight_cube = jnp.asarray(weight_np, jnp.float32)
    weight_block = weight_cube.reshape(NP, NP, NP)
    diag_ids = np.arange(NP ** 3)
    stiff_diag = jnp.asarray(stiff_np[diag_ids, diag_ids], jnp.float32)
    cell_index = (jnp.arange(N_DOM, dtype=jnp.int32)[:, None] * E_DEV + element_order.astype(jnp.int32)).reshape(-1).astype(jnp.int32)
    layer_total = N_DOM * BZ

    def shared(values):
        leading = values.shape[:-2]
        brick_values = jnp.zeros_like(values).at[..., cell_index, :].set(values)
        brick_values = brick_values.reshape(leading + (layer_total, BY, BX, NP, NP, NP))
        pair_sum = brick_values[..., :-1, :, :, -1] + brick_values[..., 1:, :, :, 0]
        brick_values = brick_values.at[..., :-1, :, :, -1].set(pair_sum).at[..., 1:, :, :, 0].set(pair_sum)
        pair_sum = brick_values[..., :-1, :, :, -1, :] + brick_values[..., 1:, :, :, 0, :]
        brick_values = brick_values.at[..., :-1, :, :, -1, :].set(pair_sum).at[..., 1:, :, :, 0, :].set(pair_sum)
        pair_sum = brick_values[..., :-1, :, :, -1, :, :] + brick_values[..., 1:, :, :, 0, :, :]
        brick_values = brick_values.at[..., :-1, :, :, -1, :, :].set(pair_sum).at[..., 1:, :, :, 0, :, :].set(pair_sum)
        return brick_values.reshape(leading + (ELEMS, NODES))[..., cell_index, :]

    def derivatives(values):
        node_cube = values.reshape(ELEMS, NP, NP, NP)
        first_dir = jnp.einsum("ai,ekji->ekja", diff_matrix, node_cube, precision=highest)
        second_dir = jnp.einsum("aj,ekji->ekai", diff_matrix, node_cube, precision=highest)
        third_dir = jnp.einsum("ak,ekji->eaji", diff_matrix, node_cube, precision=highest)
        return [first_dir, second_dir, third_dir]

    def stiffness_apply(values):
        parts_list = derivatives(values)
        stiff_total = jnp.einsum("ai,ekja->ekji", diff_matrix, weight_block * parts_list[0], precision=highest)
        stiff_total = stiff_total + jnp.einsum("aj,ekai->ekji", diff_matrix, weight_block * parts_list[1], precision=highest)
        stiff_total = stiff_total + jnp.einsum("ak,eaji->ekji", diff_matrix, weight_block * parts_list[2], precision=highest)
        return stiff_total.reshape(ELEMS, NODES)

    def operate(values):
        return shared(viscosity[:, None] * stiffness_apply(values) + mass_coef[:, None] * (weight_cube * values))

    multiplicity = shared(jnp.ones((ELEMS, NODES), jnp.float32))
    inverse_mult = 1.0 / multiplicity

    def weighted_dot(first_vec, second_vec):
        return jnp.sum(first_vec * second_vec * inverse_mult)

    rhs_all = shared(weight_cube * forcing)
    jacobi = shared(viscosity[:, None] * stiff_diag + mass_coef[:, None] * weight_cube)
    velocity = []
    gradient_rows = []
    for component in range(3):
        solution = jnp.zeros((ELEMS, NODES), jnp.float32)
        residual = rhs_all[component]
        precond = residual / jacobi
        direction = precond
        energy_now = weighted_dot(residual, precond)
        for iteration in range(ITERS):
            image = operate(direction)
            step_size = energy_now / weighted_dot(direction, image)
            solution = solution + step_size * direction
            residual = residual - step_size * image
            precond = residual / jacobi
            energy_next = weighted_dot(residual, precond)
            direction = precond + (energy_next / energy_now) * direction
            energy_now = energy_next
        velocity.append(solution)
        grads = shared(jnp.stack([cube_values.reshape(ELEMS, NODES) for cube_values in derivatives(solution)])) * inverse_mult / NP
        rounded = lax.optimization_barrier(grads.astype(jnp.bfloat16)).astype(jnp.float32)
        gradient_rows.append([rounded[0], rounded[1], rounded[2]])
    vortex_value = lambda_two(gradient_rows)
    owner_ids = owner.astype(jnp.int32)
    matches = (owner_ids[:, :, None] == jnp.arange(N_DOM, dtype=jnp.int32)[None, None, :]).astype(jnp.int32)
    running = jnp.cumsum(matches, axis=1)
    slot_rank = jnp.sum(matches * running, axis=2) - 1
    partition = jnp.arange(N_DOM, dtype=jnp.int32)[:, None]
    dest_row = jnp.where(owner_ids >= 0, owner_ids * E_DEV + partition * CAP + slot_rank, ELEMS).reshape(-1).astype(jnp.int32)
    analysis = jnp.zeros((ELEMS, NODES), jnp.float32).at[dest_row].set(vortex_value, mode="drop")
    return jnp.concatenate([jnp.stack(velocity), analysis[None]], 0)
```

```python
import jax
import jax.numpy as jnp
import numpy as np
from jax import lax
from jax.experimental import pallas as pl
from jax.experimental.pallas import tpu as pltpu
from jax.sharding import PartitionSpec as P

NP = 8
BX = 8
BY = 8
ITERS = 4
SWEEPS = 4
FACE = NP * NP
LAYER = BX * BY
TILE = 2 * LAYER
F32 = jnp.float32
BF16 = jnp.bfloat16


def legendre_values(points, node_count):
    legendre = np.zeros((points.shape[0], node_count))
    legendre[:, 0] = 1.0
    legendre[:, 1] = points
    for poly_order in range(2, node_count):
        legendre[:, poly_order] = (
            (2 * poly_order - 1) * points * legendre[:, poly_order - 1]
            - (poly_order - 1) * legendre[:, poly_order - 2]
        ) / poly_order
    return legendre


def lobatto_table(node_count):
    degree = node_count - 1
    points = np.cos(np.pi * np.arange(node_count) / degree)
    for attempt in range(60):
        legendre = legendre_values(points, node_count)
        points = points - (points * legendre[:, degree] - legendre[:, degree - 1]) / (
            node_count * legendre[:, degree]
        )
    points = points[::-1].copy()
    end_values = legendre_values(points, node_count)[:, degree]
    weights = 2.0 / (degree * node_count * end_values * end_values)
    spacing = points[:, None] - points[None, :] + np.eye(node_count)
    diff_matrix = end_values[:, None] / end_values[None, :] / spacing
    diff_matrix = diff_matrix * (1.0 - np.eye(node_count))
    diff_matrix[0, 0] = -degree * node_count / 4.0
    diff_matrix[-1, -1] = degree * node_count / 4.0
    return (weights, diff_matrix)


def operator_tables(node_count):
    weights, diff_matrix = lobatto_table(node_count)
    identity = np.eye(node_count)
    weight_cube = (
        weights[:, None, None] * weights[None, :, None] * weights[None, None, :]
    ).reshape(-1)
    directional = [
        np.kron(identity, np.kron(identity, diff_matrix)),
        np.kron(identity, np.kron(diff_matrix, identity)),
        np.kron(diff_matrix, np.kron(identity, identity)),
    ]
    stiffness = np.zeros((node_count**3, node_count**3))
    for direction_matrix in directional:
        stiffness = stiffness + direction_matrix.T @ (weight_cube[:, None] * direction_matrix)
    return diff_matrix, weight_cube, stiffness


def split3_np(table):
    parts = []
    rest = np.asarray(table, np.float64)
    for _ in range(3):
        part = rest.astype(np.float32).astype(BF16)
        parts.append(part)
        rest = rest - part.astype(np.float64)
    return parts


def host_tables():
    diff_matrix, weight_cube, stiffness = operator_tables(NP)
    half = FACE * NP // 2
    flip = np.concatenate([np.arange(FACE) + FACE * k for k in range(NP - 1, NP // 2 - 1, -1)])
    top = stiffness[:half, :half]
    cross = stiffness[:half][:, flip]
    even = split3_np(0.5 * (top + cross))
    odd = split3_np(0.5 * (top - cross))
    kmat = np.stack(even + odd)
    diag = np.diag(stiffness)
    scaled = stiffness / np.sqrt(diag[:, None] * diag[None, :])
    bound = max(1.0, float(np.linalg.eigvalsh(scaled)[-1]))
    cols = np.stack([weight_cube, diag]).astype(np.float32)
    cols = np.ascontiguousarray(np.broadcast_to(cols[:, :, None], cols.shape + (TILE,)))
    dcol = np.zeros((NP, NP, TILE), np.float32)
    for shift in range(NP):
        for row in range(NP):
            dcol[shift, row] = diff_matrix[row, (row + shift) % NP]
    return diff_matrix, kmat, cols, dcol, bound


def split3(value):
    high = value.astype(BF16)
    rest = value - high.astype(F32)
    mid = rest.astype(BF16)
    low = (rest - mid.astype(F32)).astype(BF16)
    return high, mid, low


def dot_nn(a, b):
    return jnp.dot(a, b, preferred_element_type=F32)


def dot_nt(a, b):
    return lax.dot_general(a, b, (((1,), (1,)), ((), ())), preferred_element_type=F32)


def iota(shape, dim):
    return lax.broadcasted_iota(jnp.int32, shape, dim)


def wide(col, lanes):
    return jnp.concatenate([col] * (lanes // col.shape[1]), axis=1)


def prep_kernel(comp_ref, force_ref, order_ref, coef_ref, cols_ref, pack_ref):
    elems = order_ref.shape[1]
    nodes = force_ref.shape[2]
    cell_by_slot = (iota((elems, elems), 0) == order_ref[...]).astype(F32)
    perm = jnp.transpose(cell_by_slot).astype(BF16)
    chunk = 128
    for at in range(0, nodes, chunk):
        piece = jnp.transpose(force_ref[0, :, at : at + chunk])
        high, mid, low = split3(piece)
        moved = dot_nn(high, perm) + dot_nn(mid, perm) + dot_nn(low, perm)
        pack_ref[at : at + chunk, :] = wide(cols_ref[0, at : at + chunk, :], elems) * moved
    high, mid, low = split3(coef_ref[...])
    pack_ref[nodes:, :] = dot_nn(high, perm) + dot_nn(mid, perm) + dot_nn(low, perm)


def place_kernel(cap, order_ref, owner_ref, place_ref):
    elems = order_ref.shape[1]
    owners = elems // cap
    rows = max(8, owners)
    owner_row = owner_ref[...]
    match = (iota((rows, elems), 0) == owner_row).astype(F32)
    before = (iota((elems, elems), 0) < iota((elems, elems), 1)).astype(BF16)
    running = dot_nn(match.astype(BF16), before)
    rank = jnp.sum(match * running, axis=0, keepdims=True).astype(jnp.int32)
    dest = jnp.where(owner_row >= 0, owner_row * cap + rank, -1)
    to_dest = (iota((elems, elems), 0) == dest).astype(BF16)
    cell_by_slot = (iota((elems, elems), 0) == order_ref[...]).astype(BF16)
    place_ref[...] = dot_nt(to_dest, cell_by_slot).astype(BF16)


def lane_masks(rows):
    lane = iota((rows, TILE), 1)
    x_pos = lane % BX
    y_pos = lane // BX % BY
    return x_pos < BX - 1, x_pos > 0, y_pos < BY - 1, y_pos > 0, lane < LAYER


def pair(first, second, keep, back, stride, scale):
    up = pltpu.roll(first, TILE - stride, 1)
    down = pltpu.roll(second, stride, 1)
    if scale is None:
        return first + jnp.where(back, down, 0.0), second + jnp.where(keep, up, 0.0)
    return (
        jnp.where(back, scale * (first + down), first),
        jnp.where(keep, scale * (second + up), second),
    )


def share_xy(ref, tiles, scale=None):
    x_keep, x_back, y_keep, y_back, _ = lane_masks(FACE)
    y_keep, y_back = y_keep[:NP], y_back[:NP]
    for t in tiles:
        low = ref[t, pl.ds(0, FACE, stride=NP), :]
        high = ref[t, pl.ds(NP - 1, FACE, stride=NP), :]
        low, high = pair(low, high, x_keep, x_back, 1, scale)
        ref[t, pl.ds(0, FACE, stride=NP), :] = low
        ref[t, pl.ds(NP - 1, FACE, stride=NP), :] = high
        for k in range(NP):
            first = pl.ds(k * FACE, NP)
            last = pl.ds(k * FACE + FACE - NP, NP)
            low, high = pair(ref[t, first, :], ref[t, last, :], y_keep, y_back, BX, scale)
            ref[t, first, :] = low
            ref[t, last, :] = high


def load_block(ref, n, rows):
    return jnp.concatenate([ref[2 * n, rows, :], ref[2 * n + 1, rows, :]], axis=1)


def save_block(ref, n, rows, value):
    ref[2 * n, rows, :] = value[:, :TILE]
    ref[2 * n + 1, rows, :] = value[:, TILE:]


def share_z(ref, tiles):
    lower = lane_masks(FACE)[4]
    first = pl.ds(0, FACE)
    last = pl.ds((NP - 1) * FACE, FACE)
    lows = [ref[t, first, :] for t in tiles]
    highs = [ref[t, last, :] for t in tiles]
    low_roll = [pltpu.roll(v, LAYER, 1) for v in lows] + [jnp.zeros((FACE, TILE), F32)]
    high_roll = [jnp.zeros((FACE, TILE), F32)] + [pltpu.roll(v, LAYER, 1) for v in highs]
    for n, t in enumerate(tiles):
        up = jnp.where(lower, low_roll[n], low_roll[n + 1])
        down = jnp.where(lower, high_roll[n], high_roll[n + 1])
        ref[t, last, :] = highs[n] + up
        ref[t, first, :] = lows[n] + down


def krylov_kernel(
    diff, bound, meta_ref, own_ref, a_ref, b_ref, kmat_ref, cols_ref,
    basis_ref, near_ref, face_ref, dots_ref,
    work, coef, inv, vec, ghost, even, odd, prod,
):
    nodes = cols_ref.shape[1]
    elems = own_ref.shape[1]
    half = nodes // 2
    steps = ITERS
    odd_part = meta_ref[1] > 0
    wide_tile = pl.ds(0, TILE)
    high_tile = pl.ds(TILE, TILE)

    def gather(rows, out_own, out_near, out_far):
        out_own(own_ref[rows, :])
        a_low, a_high = a_ref[rows, wide_tile], a_ref[rows, high_tile]
        b_low, b_high = b_ref[rows, wide_tile], b_ref[rows, high_tile]
        out_near(
            jnp.where(odd_part, a_high, b_high), jnp.where(odd_part, b_low, a_low)
        )
        out_far(
            jnp.where(odd_part, a_low, b_low), jnp.where(odd_part, b_high, a_high)
        )

    def store(ref, n, rows):
        def put(*parts):
            save_block(ref, n, rows, parts[0] if len(parts) == 1 else jnp.concatenate(parts, axis=1))
        return put

    def store_coef(n):
        def put(*parts):
            coef[n] = parts[0] if len(parts) == 1 else jnp.concatenate(parts, axis=1)
        return put

    tail = pl.ds(nodes, own_ref.shape[0] - nodes)
    gather(tail, store_coef(0), store_coef(1), store_coef(2))

    @pl.loop(0, NP)
    def _(k):
        rows = pl.ds(pl.multiple_of(k * FACE, FACE), FACE)
        gather(rows, store(work, 0, rows), store(work, 1, rows), store(work, 2, rows))
        w_col = wide(cols_ref[0, rows, :], elems)
        d_col = wide(cols_ref[1, rows, :], elems)
        for n in range(3):
            save_block(inv, n, rows, coef[n, 0:1, :] * d_col + coef[n, 1:2, :] * w_col)

    far_tiles = [4, 2, 0, 1, 3, 5]
    near_tiles = far_tiles[1:5]
    share_xy(work, far_tiles)
    share_z(work, far_tiles)
    share_xy(inv, far_tiles)
    share_z(inv, far_tiles)

    @pl.loop(0, NP)
    def _(k):
        rows = pl.ds(pl.multiple_of(k * FACE, FACE), FACE)
        for n in range(3):
            total = load_block(inv, n, rows)
            recip = jnp.where(total > 0.0, 1.0 / total, 0.0)
            save_block(inv, n, rows, recip)
            value = recip * load_block(work, n, rows)
            if n == 0:
                basis_ref[0, rows, :] = value
            elif n == 1:
                ghost[0, rows, :] = value
            else:
                vec[rows, :] = value

    def vector(m, n, rows):
        if n == 0:
            return basis_ref[m, rows, :]
        return ghost[m, rows, :] if n == 1 else vec[rows, :]

    dots_ref[...] = jnp.zeros_like(dots_ref)

    def fold(value):
        rows, lanes = value.shape
        total = jnp.sum(value.reshape(rows // 8, 8, lanes), axis=0)
        return sum(total[:, at : at + TILE] for at in range(0, lanes, TILE))

    def apply(m, n):
        @pl.loop(0, NP // 2)
        def _(k):
            top = pl.ds(pl.multiple_of(k * FACE, FACE), FACE)
            bottom = pl.ds(pl.multiple_of((NP - 1 - k) * FACE, FACE), FACE)
            v_top = vector(m, n, top)
            v_bottom = vector(m, n, bottom)
            for part, ref in ((v_top + v_bottom, even), (v_top - v_bottom, odd)):
                high, mid, low = split3(part)
                ref[0, top, :] = high
                ref[1, top, :] = mid
                ref[2, top, :] = low

        for parity, ref in ((0, even), (1, odd)):
            base = 3 * parity
            prod[parity] = (
                dot_nn(kmat_ref[base], ref[2])
                + dot_nn(kmat_ref[base + 1], ref[1])
                + dot_nn(kmat_ref[base + 2], ref[0])
                + dot_nn(kmat_ref[base], ref[1])
                + dot_nn(kmat_ref[base + 1], ref[0])
                + dot_nn(kmat_ref[base], ref[0])
            )

        @pl.loop(0, NP // 2)
        def _(k):
            top = pl.ds(pl.multiple_of(k * FACE, FACE), FACE)
            bottom = pl.ds(pl.multiple_of((NP - 1 - k) * FACE, FACE), FACE)
            p_even = prod[0, top, :]
            p_odd = prod[1, top, :]
            w_top = wide(cols_ref[0, top, :], elems)
            w_bottom = wide(cols_ref[0, bottom, :], elems)
            visc = coef[n, 0:1, :]
            mass = coef[n, 1:2, :]
            q_top = visc * (p_even + p_odd) + mass * (w_top * vector(m, n, top))
            q_bottom = visc * (p_even - p_odd) + mass * (w_bottom * vector(m, n, bottom))
            if m + 1 < steps:
                save_block(work, n, top, q_top)
                save_block(work, n, bottom, q_bottom)
            if n == 0:
                for i in range(m + 1):
                    dots_ref[m * (m + 1) // 2 + i] += fold(
                        basis_ref[i, top, :] * q_top + basis_ref[i, bottom, :] * q_bottom
                    )
                at = steps * (steps + 1) // 2 + m
                dots_ref[at] += fold(
                    basis_ref[m, top, :] * own_ref[top, :]
                    + basis_ref[m, bottom, :] * own_ref[bottom, :]
                )

    for m in range(steps):
        if m + 1 == steps:
            apply(m, 0)
            continue
        blocks = (0, 1, 2) if m == 0 else (0, 1)
        for n in blocks:
            apply(m, n)
        tiles = far_tiles if m == 0 else near_tiles
        share_xy(work, tiles)
        share_z(work, tiles)
        outs = (0, 1) if m + 2 < steps else (0,)

        @pl.loop(0, NP)
        def _(k):
            rows = pl.ds(pl.multiple_of(k * FACE, FACE), FACE)
            for n in outs:
                value = (2.0 / bound) * (load_block(inv, n, rows) * load_block(work, n, rows)) - vector(m, n, rows)
                if m > 0:
                    value = value + value - vector(m - 1, n, rows)
                if n == 0:
                    basis_ref[m + 1, rows, :] = value
                else:
                    ghost[m + 1, rows, :] = value

    def plane(load, row):
        total = None
        for k in range(NP):
            term = float(diff[row, k]) * load(k)
            total = term if total is None else total + term
        return total

    lower = lane_masks(FACE)[4]

    def rows_of(k):
        return pl.ds(k * FACE, FACE)

    last = steps - 1
    bottom = plane(lambda k: basis_ref[last, rows_of(k), wide_tile], 0)
    top = plane(lambda k: basis_ref[last, rows_of(k), high_tile], NP - 1)
    face_ref[...] = jnp.where(lower, bottom, top)
    for m in range(steps - 1):
        below = plane(lambda k: ghost[m, rows_of(k), wide_tile], NP - 1)
        above = plane(lambda k: ghost[m, rows_of(k), high_tile], 0)
        near_ref[m] = jnp.where(lower, above, below)


def solve_coefficients(sums):
    size = ITERS
    gram = {}
    for j in range(size):
        for i in range(j + 1):
            at = j * (j + 1) // 2 + i
            gram[j, i] = sums[at : at + 1]
    at = size * (size + 1) // 2
    right = [sums[at + i : at + i + 1] for i in range(size)]
    lower, recip = {}, []
    reduced = {}
    for k in range(size):
        for i in range(k, size):
            value = gram[i, k]
            for m in range(k):
                value = value - lower[i, m] * reduced[k, m]
            reduced[i, k] = value
        pivot = reduced[k, k]
        usable = pivot > 1e-7 * gram[k, k]
        inverse = jnp.where(usable, 1.0 / jnp.where(usable, pivot, 1.0), 0.0)
        recip.append(inverse)
        for i in range(k + 1, size):
            lower[i, k] = reduced[i, k] * inverse
    for k in range(size):
        for m in range(k):
            right[k] = right[k] - lower[k, m] * right[m]
    out = [None] * size
    for k in reversed(range(size)):
        value = right[k] * recip[k]
        for m in range(k + 1, size):
            value = value - lower[m, k] * out[m]
        out[k] = value
    return out


def gradient_kernel(
    diff, meta_ref, dots_ref, basis_ref, near_ref, fa_ref, fb_ref, dcol_ref,
    grad_ref, vel_ref, work,
):
    elems = basis_ref.shape[2]
    quarters = grad_ref.shape[0]
    quarter = grad_ref.shape[2]
    scalars = jnp.sum(dots_ref[...], axis=1, keepdims=True)
    weights = solve_coefficients(scalars)
    tiles = range(elems // TILE)

    @pl.loop(0, NP)
    def _(k):
        rows = pl.ds(pl.multiple_of(k * FACE, FACE), FACE)
        total = weights[0] * basis_ref[0, rows, :]
        for m in range(1, ITERS):
            total = total + weights[m] * basis_ref[m, rows, :]
        vel_ref[rows, :] = total

    lower = lane_masks(FACE)[4]
    x_keep, x_back, y_keep, y_back, _ = lane_masks(FACE)
    odd_part = meta_ref[1] > 0
    from_above = jnp.where(odd_part, fb_ref[...], fa_ref[...])
    from_below = jnp.where(odd_part, fa_ref[...], fb_ref[...])
    near = weights[ITERS - 1] * jnp.where(lower, from_above, from_below)
    for m in range(ITERS - 1):
        near = near + weights[m] * near_ref[m]
    near = pltpu.roll(near, LAYER, 1)

    def finish(direction, scale):
        share_xy(work, tiles, 0.5)
        if direction == 2:
            first = pl.ds(0, FACE)
            last = pl.ds((NP - 1) * FACE, FACE)
            lows = [work[t, first, :] for t in tiles]
            highs = [work[t, last, :] for t in tiles]
            low_roll = [pltpu.roll(v, LAYER, 1) for v in lows] + [near]
            high_roll = [near] + [pltpu.roll(v, LAYER, 1) for v in highs]
            count = len(tiles)
            for n in tiles:
                up = jnp.where(lower, low_roll[n], low_roll[n + 1])
                down = jnp.where(lower, high_roll[n], high_roll[n + 1])
                high_mean = 0.5 * (highs[n] + up)
                low_mean = 0.5 * (lows[n] + down)
                if n == count - 1:
                    edge = jnp.logical_and(jnp.logical_not(lower), meta_ref[3] > 0)
                    high_mean = jnp.where(edge, highs[n], high_mean)
                if n == 0:
                    edge = jnp.logical_and(lower, meta_ref[2] > 0)
                    low_mean = jnp.where(edge, lows[n], low_mean)
                work[n, last, :] = high_mean
                work[n, first, :] = low_mean
        for q in range(quarters):
            grad_ref[q, direction] = (load_block(work, 0, pl.ds(q * quarter, quarter)) * scale).astype(BF16)

    @pl.loop(0, NP)
    def _(k):
        rows = pl.ds(pl.multiple_of(k * FACE, FACE), FACE)
        value = vel_ref[rows, :].reshape(NP, NP, elems)
        total = wide(dcol_ref[0], elems)[None] * value
        for shift in range(1, NP):
            total = total + wide(dcol_ref[shift], elems)[None] * pltpu.roll(value, NP - shift, 1)
        save_block(work, 0, rows, total.reshape(FACE, elems))

    finish(0, 1.0 / NP)

    @pl.loop(0, NP)
    def _(k):
        rows = pl.ds(pl.multiple_of(k * FACE, FACE), FACE)
        value = vel_ref[rows, :].reshape(NP, NP, elems)
        for j in range(NP):
            total = float(diff[j, 0]) * value[0]
            for m in range(1, NP):
                total = total + float(diff[j, m]) * value[m]
            save_block(work, 0, pl.ds(pl.multiple_of(k * FACE + j * NP, NP), NP), total)

    finish(1, 1.0 / NP)

    @pl.loop(0, NP)
    def _(j):
        planes = [vel_ref[pl.ds(pl.multiple_of(m * FACE + j * NP, NP), NP), :] for m in range(NP)]
        for k in range(NP):
            total = float(diff[k, 0]) * planes[0]
            for m in range(1, NP):
                total = total + float(diff[k, m]) * planes[m]
            save_block(work, 0, pl.ds(pl.multiple_of(k * FACE + j * NP, NP), NP), total)

    finish(2, 1.0 / NP)


def slots_kernel(order_ref, vel_ref, out_ref):
    elems = order_ref.shape[1]
    cell_by_slot = (iota((elems, elems), 0) == order_ref[...]).astype(F32)
    pick = jnp.transpose(cell_by_slot).astype(BF16)
    high, mid, low = split3(vel_ref[...])
    out_ref[...] = dot_nt(pick, high) + dot_nt(pick, mid) + dot_nt(pick, low)


def middle_eigenvalue(jac):
    strain = [[0.5 * (jac[a][b] + jac[b][a]) for b in range(3)] for a in range(3)]
    spin = [[0.5 * (jac[a][b] - jac[b][a]) for b in range(3)] for a in range(3)]
    mat = [[None] * 3 for _ in range(3)]
    for a in range(3):
        for b in range(a, 3):
            total = strain[a][0] * strain[0][b] + spin[a][0] * spin[0][b]
            for c in (1, 2):
                total = total + strain[a][c] * strain[c][b] + spin[a][c] * spin[c][b]
            mat[a][b] = total
            mat[b][a] = total
    for _ in range(SWEEPS):
        for p, q, r in ((0, 1, 2), (0, 2, 1), (1, 2, 0)):
            pivot = mat[p][q]
            first, second = mat[p][p], mat[q][q]
            num = 2.0 * pivot
            den = first - second
            size = jnp.maximum(jnp.abs(num), jnp.abs(den))
            safe = jnp.where(size > 0.0, size, 1.0)
            num_s = num / safe
            den_s = den / safe
            inv_norm = lax.rsqrt(jnp.where(size > 0.0, num_s * num_s + den_s * den_s, 1.0))
            cos_two = jnp.where(size > 0.0, den_s * inv_norm, 1.0)
            sin_two = num_s * inv_norm
            big = jnp.sqrt(0.5 + 0.5 * jnp.abs(cos_two))
            small = 0.5 * sin_two / big
            forward = cos_two >= 0.0
            sign = jnp.where(num < 0.0, -1.0, 1.0)
            cosine = jnp.where(forward, big, jnp.abs(small))
            sine = jnp.where(forward, small, sign * big)
            cross = 2.0 * cosine * sine * pivot
            cc, ss = cosine * cosine, sine * sine
            side_p, side_q = mat[r][p], mat[r][q]
            mat[p][p] = cc * first + cross + ss * second
            mat[q][q] = ss * first - cross + cc * second
            zero = jnp.zeros_like(pivot)
            mat[p][q] = mat[q][p] = zero
            mat[r][p] = mat[p][r] = cosine * side_p + sine * side_q
            mat[r][q] = mat[q][r] = cosine * side_q - sine * side_p
    d0, d1, d2 = mat[0][0], mat[1][1], mat[2][2]
    largest = jnp.maximum(jnp.maximum(d0, d1), d2)
    smallest = jnp.minimum(jnp.minimum(d0, d1), d2)
    return d0 + d1 + d2 - largest - smallest


def vortex_kernel(grad_ref, place_ref, out_ref, value):
    rows_all = grad_ref.shape[2]
    step = 16

    @pl.loop(0, rows_all // step)
    def _(n):
        rows = pl.ds(pl.multiple_of(n * step, step), step)
        jac = [[grad_ref[c, d, rows, :].astype(F32) for d in range(3)] for c in range(3)]
        value[rows, :] = middle_eigenvalue(jac)

    high, mid, low = split3(value[...])
    place = place_ref[...]
    moved = dot_nt(place, high) + dot_nt(place, mid) + dot_nt(place, low)
    out_ref[...] = moved.reshape(out_ref.shape)


def final_kernel(meta_ref, vortex_ref, vel_ref, out_ref):
    quarters = vortex_ref.shape[0]
    quarter = vortex_ref.shape[2]

    @pl.when(meta_ref[4] > 0)
    def _():
        for q in range(quarters):
            out_ref[0, :, q * quarter : (q + 1) * quarter] = vortex_ref[q]

    @pl.when(meta_ref[4] == 0)
    def _():
        out_ref[0] = vel_ref[...]


def vmem():
    return pl.BlockSpec(memory_space=pltpu.VMEM)


def smem():
    return pl.BlockSpec(memory_space=pltpu.SMEM)


def cost(flops, size):
    return pl.CostEstimate(flops=flops, bytes_accessed=size, transcendentals=0)


def per_device(forcing, viscosity, mass_coef, element_order, owner):
    elems = viscosity.shape[0]
    nodes = forcing.shape[2]
    parts = lax.axis_size("dom")
    groups = lax.axis_size("grp")
    part = lax.axis_index("dom")
    group = lax.axis_index("grp")
    cap = elems // parts
    quarter = nodes // groups
    diff, kmat_np, cols_np, dcol_np, bound = host_tables()
    kmat = jnp.asarray(kmat_np, BF16)
    cols = jnp.asarray(cols_np)
    dcol = jnp.asarray(dcol_np)
    meta = jnp.stack(
        [
            jnp.minimum(group, 2),
            part % 2,
            (part == 0).astype(jnp.int32),
            (part == parts - 1).astype(jnp.int32),
            (group == groups - 1).astype(jnp.int32),
        ]
    ).astype(jnp.int32)
    coef = jnp.concatenate(
        [viscosity[None], mass_coef[None], jnp.zeros((6, elems), F32)], axis=0
    )
    sds = jax.ShapeDtypeStruct

    pack = pl.pallas_call(
        prep_kernel,
        grid_spec=pltpu.PrefetchScalarGridSpec(
            num_scalar_prefetch=1,
            grid=(1,),
            in_specs=[
                pl.BlockSpec((1, elems, nodes), lambda n, m: (m[0], 0, 0)),
                pl.BlockSpec((1, elems), lambda n, m: (0, 0)),
                pl.BlockSpec((8, elems), lambda n, m: (0, 0)),
                pl.BlockSpec((2, nodes, TILE), lambda n, m: (0, 0, 0)),
            ],
            out_specs=pl.BlockSpec((nodes + 8, elems), lambda n, m: (0, 0)),
        ),
        out_shape=sds((nodes + 8, elems), F32),
        cost_estimate=cost(10**9, 2 * 10**6),
        name="prep",
    )(meta, forcing, element_order, coef, cols)

    swap_a = [(i, i ^ 1) for i in range(parts) if i ^ 1 < parts]
    swap_b = [(i, ((i - 1) ^ 1) + 1) for i in range(1, parts - 1)]
    ghost_a = lax.ppermute(pack, "dom", swap_a)
    ghost_b = lax.ppermute(pack, "dom", swap_b)

    place = pl.pallas_call(
        lambda *refs: place_kernel(cap, *refs),
        in_specs=[vmem(), vmem()],
        out_specs=vmem(),
        out_shape=sds((elems, elems), BF16),
        cost_estimate=cost(10**9, 2 * 10**6),
        name="place",
    )(element_order, owner)

    basis, near, face, dots = pl.pallas_call(
        lambda *refs: krylov_kernel(diff, bound, *refs),
        in_specs=[smem()] + [vmem()] * 5,
        out_specs=[vmem()] * 4,
        out_shape=[
            sds((ITERS, nodes, elems), F32),
            sds((ITERS - 1, FACE, TILE), F32),
            sds((FACE, TILE), F32),
            sds((16, 8, TILE), F32),
        ],
        scratch_shapes=[
            pltpu.VMEM((6, nodes, TILE), F32),
            pltpu.VMEM((3, 8, elems), F32),
            pltpu.VMEM((6, nodes, TILE), F32),
            pltpu.VMEM((nodes, elems), F32),
            pltpu.VMEM((ITERS - 1, nodes, elems), F32),
            pltpu.VMEM((3, nodes // 2, elems), BF16),
            pltpu.VMEM((3, nodes // 2, elems), BF16),
            pltpu.VMEM((2, nodes // 2, elems), F32),
        ],
        cost_estimate=cost(10**10, 10**7),
        name="krylov",
    )(meta, pack, ghost_a, ghost_b, kmat, cols)

    message = jnp.concatenate([face, jnp.sum(dots, axis=1)], axis=0)
    face_a = lax.ppermute(message, "dom", swap_a)
    face_b = lax.ppermute(face, "dom", swap_b)
    sums = message[FACE:] + face_a[FACE:]
    reach = 2
    while reach < parts:
        sums = sums + lax.ppermute(sums, "dom", [(i, i ^ reach) for i in range(parts)])
        reach *= 2

    grads, vel = pl.pallas_call(
        lambda *refs: gradient_kernel(diff, *refs),
        in_specs=[smem()] + [vmem()] * 6,
        out_specs=[vmem()] * 2,
        out_shape=[sds((groups, 3, quarter, elems), BF16), sds((nodes, elems), F32)],
        scratch_shapes=[pltpu.VMEM((2, nodes, TILE), F32)],
        cost_estimate=cost(10**9, 4 * 10**6),
        name="gradient",
    )(meta, sums, basis, near, face_a[:FACE], face_b, dcol)

    exchanged = lax.all_to_all(grads, "grp", split_axis=0, concat_axis=0, tiled=True)

    vel_slot = pl.pallas_call(
        slots_kernel,
        in_specs=[vmem(), vmem()],
        out_specs=vmem(),
        out_shape=sds((elems, nodes), F32),
        cost_estimate=cost(10**9, 2 * 10**6),
        name="slots",
    )(element_order, vel)

    packed = pl.pallas_call(
        vortex_kernel,
        in_specs=[vmem(), vmem()],
        out_specs=vmem(),
        out_shape=sds((parts, cap, quarter), F32),
        scratch_shapes=[pltpu.VMEM((quarter, elems), F32)],
        cost_estimate=cost(10**9, 2 * 10**6),
        name="vortex",
    )(exchanged, place)

    padding = jnp.zeros(((groups - 1) * parts, cap, quarter), F32)
    received = lax.all_to_all(
        jnp.concatenate([padding, packed], 0),
        ("grp", "dom"),
        split_axis=0,
        concat_axis=0,
        tiled=True,
    )
    return pl.pallas_call(
        final_kernel,
        in_specs=[smem(), vmem(), vmem()],
        out_specs=vmem(),
        out_shape=sds((1, elems, nodes), F32),
        cost_estimate=cost(10**6, 2 * 10**6),
        name="final",
    )(meta, received.reshape(groups, elems, quarter), vel_slot)


def solution(mesh):
    in_specs = (P(None, "dom", None), P("dom"), P("dom"), P("dom", None), P("dom", None))
    out_specs = P("grp", "dom", None)
    return jax.shard_map(
        per_device, mesh=mesh, in_specs=in_specs, out_specs=out_specs, check_vma=False
    )
```

```python
import jax
import jax.numpy as jnp
import numpy as np
from jax import lax
from jax.experimental import pallas as pl
from jax.experimental.pallas import tpu as pltpu
from jax.sharding import PartitionSpec as P

NP = 8
BX = 8
BY = 8
ITERS = 4
SWEEPS = 4
FACE = NP * NP
LAYER = BX * BY
TILE = 2 * LAYER
F32 = jnp.float32
BF16 = jnp.bfloat16


def legendre_values(points, node_count):
    legendre = np.zeros((points.shape[0], node_count))
    legendre[:, 0] = 1.0
    legendre[:, 1] = points
    for poly_order in range(2, node_count):
        legendre[:, poly_order] = (
            (2 * poly_order - 1) * points * legendre[:, poly_order - 1]
            - (poly_order - 1) * legendre[:, poly_order - 2]
        ) / poly_order
    return legendre


def lobatto_table(node_count):
    degree = node_count - 1
    points = np.cos(np.pi * np.arange(node_count) / degree)
    for attempt in range(60):
        legendre = legendre_values(points, node_count)
        points = points - (points * legendre[:, degree] - legendre[:, degree - 1]) / (
            node_count * legendre[:, degree]
        )
    points = points[::-1].copy()
    end_values = legendre_values(points, node_count)[:, degree]
    weights = 2.0 / (degree * node_count * end_values * end_values)
    spacing = points[:, None] - points[None, :] + np.eye(node_count)
    diff_matrix = end_values[:, None] / end_values[None, :] / spacing
    diff_matrix = diff_matrix * (1.0 - np.eye(node_count))
    diff_matrix[0, 0] = -degree * node_count / 4.0
    diff_matrix[-1, -1] = degree * node_count / 4.0
    return (weights, diff_matrix)


def operator_tables(node_count):
    weights, diff_matrix = lobatto_table(node_count)
    identity = np.eye(node_count)
    weight_cube = (
        weights[:, None, None] * weights[None, :, None] * weights[None, None, :]
    ).reshape(-1)
    directional = [
        np.kron(identity, np.kron(identity, diff_matrix)),
        np.kron(identity, np.kron(diff_matrix, identity)),
        np.kron(diff_matrix, np.kron(identity, identity)),
    ]
    stiffness = np.zeros((node_count**3, node_count**3))
    for direction_matrix in directional:
        stiffness = stiffness + direction_matrix.T @ (weight_cube[:, None] * direction_matrix)
    return diff_matrix, weight_cube, stiffness


def split3_np(table):
    parts = []
    rest = np.asarray(table, np.float64)
    for _ in range(3):
        part = rest.astype(np.float32).astype(BF16)
        parts.append(part)
        rest = rest - part.astype(np.float64)
    return parts


def host_tables():
    diff_matrix, weight_cube, stiffness = operator_tables(NP)
    half = FACE * NP // 2
    flip = np.concatenate([np.arange(FACE) + FACE * k for k in range(NP - 1, NP // 2 - 1, -1)])
    top = stiffness[:half, :half]
    cross = stiffness[:half][:, flip]
    even = split3_np(0.5 * (top + cross))
    odd = split3_np(0.5 * (top - cross))
    kmat = np.stack(even + odd)
    diag = np.diag(stiffness)
    scaled = stiffness / np.sqrt(diag[:, None] * diag[None, :])
    bound = max(1.0, float(np.linalg.eigvalsh(scaled)[-1]))
    cols = np.stack([weight_cube, diag]).astype(np.float32)
    cols = np.ascontiguousarray(np.broadcast_to(cols[:, :, None], cols.shape + (TILE,)))
    dcol = np.zeros((NP, NP, TILE), np.float32)
    for shift in range(NP):
        for row in range(NP):
            dcol[shift, row] = diff_matrix[row, (row + shift) % NP]
    return diff_matrix, kmat, cols, dcol, bound


def split3(value):
    high = value.astype(BF16)
    rest = value - high.astype(F32)
    mid = rest.astype(BF16)
    low = (rest - mid.astype(F32)).astype(BF16)
    return high, mid, low


def dot_nn(a, b):
    return jnp.dot(a, b, preferred_element_type=F32)


def dot_nt(a, b):
    return lax.dot_general(a, b, (((1,), (1,)), ((), ())), preferred_element_type=F32)


def iota(shape, dim):
    return lax.broadcasted_iota(jnp.int32, shape, dim)


def wide(col, lanes):
    return jnp.concatenate([col] * (lanes // col.shape[1]), axis=1)


def prep_kernel(force_any, order_ref, visc_ref, mass_ref, cols_ref, pack_ref, force_ref, sem):
    elems = order_ref.shape[1]
    nodes = force_any.shape[2]
    component = jnp.minimum(lax.axis_index("grp"), 2)
    fetch = pltpu.make_async_copy(force_any.at[component], force_ref, sem)
    fetch.start()
    cell_by_slot = (iota((elems, elems), 0) == order_ref[...]).astype(F32)
    perm = jnp.transpose(cell_by_slot).astype(BF16)
    coef = jnp.concatenate([visc_ref[...], mass_ref[...], jnp.zeros((6, elems), F32)], axis=0)
    high, mid, low = split3(coef)
    pack_ref[nodes:, :] = dot_nn(high, perm) + dot_nn(mid, perm) + dot_nn(low, perm)
    fetch.wait()
    chunk = 128
    for at in range(0, nodes, chunk):
        piece = jnp.transpose(force_ref[:, at : at + chunk])
        high, mid, low = split3(piece)
        moved = dot_nn(high, perm) + dot_nn(mid, perm) + dot_nn(low, perm)
        pack_ref[at : at + chunk, :] = wide(cols_ref[0, at : at + chunk, :], elems) * moved


def place_kernel(cap, order_ref, owner_ref, place_ref):
    elems = order_ref.shape[1]
    owners = elems // cap
    rows = max(8, owners)
    owner_row = owner_ref[...]
    match = (iota((rows, elems), 0) == owner_row).astype(F32)
    before = (iota((elems, elems), 0) < iota((elems, elems), 1)).astype(BF16)
    running = dot_nn(match.astype(BF16), before)
    rank = jnp.sum(match * running, axis=0, keepdims=True).astype(jnp.int32)
    dest = jnp.where(owner_row >= 0, owner_row * cap + rank, -1)
    to_dest = (iota((elems, elems), 0) == dest).astype(BF16)
    cell_by_slot = (iota((elems, elems), 0) == order_ref[...]).astype(BF16)
    place_ref[...] = dot_nt(to_dest, cell_by_slot).astype(BF16)


def lane_masks(rows):
    lane = iota((rows, TILE), 1)
    x_pos = lane % BX
    y_pos = lane // BX % BY
    return x_pos < BX - 1, x_pos > 0, y_pos < BY - 1, y_pos > 0, lane < LAYER


def pair(first, second, keep, back, stride, scale):
    up = pltpu.roll(first, TILE - stride, 1)
    down = pltpu.roll(second, stride, 1)
    if scale is None:
        return first + jnp.where(back, down, 0.0), second + jnp.where(keep, up, 0.0)
    return (
        jnp.where(back, scale * (first + down), first),
        jnp.where(keep, scale * (second + up), second),
    )


def share_xy(ref, tiles, scale=None):
    x_keep, x_back, y_keep, y_back, _ = lane_masks(FACE)
    y_keep, y_back = y_keep[:NP], y_back[:NP]
    for t in tiles:
        low = ref[t, pl.ds(0, FACE, stride=NP), :]
        high = ref[t, pl.ds(NP - 1, FACE, stride=NP), :]
        low, high = pair(low, high, x_keep, x_back, 1, scale)
        ref[t, pl.ds(0, FACE, stride=NP), :] = low
        ref[t, pl.ds(NP - 1, FACE, stride=NP), :] = high
        for k in range(NP):
            first = pl.ds(k * FACE, NP)
            last = pl.ds(k * FACE + FACE - NP, NP)
            low, high = pair(ref[t, first, :], ref[t, last, :], y_keep, y_back, BX, scale)
            ref[t, first, :] = low
            ref[t, last, :] = high


def load_block(ref, n, rows):
    return jnp.concatenate([ref[2 * n, rows, :], ref[2 * n + 1, rows, :]], axis=1)


def save_block(ref, n, rows, value):
    ref[2 * n, rows, :] = value[:, :TILE]
    ref[2 * n + 1, rows, :] = value[:, TILE:]


def share_z(ref, tiles):
    lower = lane_masks(FACE)[4]
    first = pl.ds(0, FACE)
    last = pl.ds((NP - 1) * FACE, FACE)
    lows = [ref[t, first, :] for t in tiles]
    highs = [ref[t, last, :] for t in tiles]
    low_roll = [pltpu.roll(v, LAYER, 1) for v in lows] + [jnp.zeros((FACE, TILE), F32)]
    high_roll = [jnp.zeros((FACE, TILE), F32)] + [pltpu.roll(v, LAYER, 1) for v in highs]
    for n, t in enumerate(tiles):
        up = jnp.where(lower, low_roll[n], low_roll[n + 1])
        down = jnp.where(lower, high_roll[n], high_roll[n + 1])
        ref[t, last, :] = highs[n] + up
        ref[t, first, :] = lows[n] + down


def krylov_kernel(
    diff, bound, own_ref, a_ref, b_ref, kmat_ref, cols_ref,
    basis_ref, near_ref, message_ref,
    work, coef, inv, vec, ghost, even, odd, prod, dots_ref,
):
    nodes = cols_ref.shape[1]
    elems = own_ref.shape[1]
    half = nodes // 2
    steps = ITERS
    odd_part = lax.axis_index("dom") % 2 > 0
    wide_tile = pl.ds(0, TILE)
    high_tile = pl.ds(TILE, TILE)

    def gather(rows, out_own, out_near, out_far):
        out_own(own_ref[rows, :])
        a_low, a_high = a_ref[rows, wide_tile], a_ref[rows, high_tile]
        b_low, b_high = b_ref[rows, wide_tile], b_ref[rows, high_tile]
        out_near(
            jnp.where(odd_part, a_high, b_high), jnp.where(odd_part, b_low, a_low)
        )
        out_far(
            jnp.where(odd_part, a_low, b_low), jnp.where(odd_part, b_high, a_high)
        )

    def store(ref, n, rows):
        def put(*parts):
            save_block(ref, n, rows, parts[0] if len(parts) == 1 else jnp.concatenate(parts, axis=1))
        return put

    def store_coef(n):
        def put(*parts):
            coef[n] = parts[0] if len(parts) == 1 else jnp.concatenate(parts, axis=1)
        return put

    tail = pl.ds(nodes, own_ref.shape[0] - nodes)
    gather(tail, store_coef(0), store_coef(1), store_coef(2))

    @pl.loop(0, NP)
    def _(k):
        rows = pl.ds(pl.multiple_of(k * FACE, FACE), FACE)
        gather(rows, store(work, 0, rows), store(work, 1, rows), store(work, 2, rows))
        w_col = wide(cols_ref[0, rows, :], elems)
        d_col = wide(cols_ref[1, rows, :], elems)
        for n in range(3):
            save_block(inv, n, rows, coef[n, 0:1, :] * d_col + coef[n, 1:2, :] * w_col)

    far_tiles = [4, 2, 0, 1, 3, 5]
    near_tiles = far_tiles[1:5]
    share_xy(work, far_tiles)
    share_z(work, far_tiles)
    share_xy(inv, far_tiles)
    share_z(inv, far_tiles)

    @pl.loop(0, NP)
    def _(k):
        rows = pl.ds(pl.multiple_of(k * FACE, FACE), FACE)
        for n in range(3):
            total = load_block(inv, n, rows)
            recip = jnp.where(total > 0.0, 1.0 / total, 0.0)
            save_block(inv, n, rows, recip)
            value = recip * load_block(work, n, rows)
            if n == 0:
                basis_ref[0, rows, :] = value
            elif n == 1:
                ghost[0, rows, :] = value
            else:
                vec[rows, :] = value

    def vector(m, n, rows):
        if n == 0:
            return basis_ref[m, rows, :]
        return ghost[m, rows, :] if n == 1 else vec[rows, :]

    dots_ref[...] = jnp.zeros_like(dots_ref)

    def fold(value):
        rows, lanes = value.shape
        total = jnp.sum(value.reshape(rows // 8, 8, lanes), axis=0)
        return sum(total[:, at : at + TILE] for at in range(0, lanes, TILE))

    def apply(m, n):
        @pl.loop(0, NP // 2)
        def _(k):
            top = pl.ds(pl.multiple_of(k * FACE, FACE), FACE)
            bottom = pl.ds(pl.multiple_of((NP - 1 - k) * FACE, FACE), FACE)
            v_top = vector(m, n, top)
            v_bottom = vector(m, n, bottom)
            for part, ref in ((v_top + v_bottom, even), (v_top - v_bottom, odd)):
                high = part.astype(BF16)
                ref[0, top, :] = high
                ref[1, top, :] = (part - high.astype(F32)).astype(BF16)

        for parity, ref in ((0, even), (1, odd)):
            base = 3 * parity
            prod[parity] = (
                dot_nn(kmat_ref[base + 1], ref[1])
                + dot_nn(kmat_ref[base + 2], ref[0])
                + dot_nn(kmat_ref[base], ref[1])
                + dot_nn(kmat_ref[base + 1], ref[0])
                + dot_nn(kmat_ref[base], ref[0])
            )

        @pl.loop(0, NP // 2)
        def _(k):
            top = pl.ds(pl.multiple_of(k * FACE, FACE), FACE)
            bottom = pl.ds(pl.multiple_of((NP - 1 - k) * FACE, FACE), FACE)
            p_even = prod[0, top, :]
            p_odd = prod[1, top, :]
            w_top = wide(cols_ref[0, top, :], elems)
            w_bottom = wide(cols_ref[0, bottom, :], elems)
            visc = coef[n, 0:1, :]
            mass = coef[n, 1:2, :]
            q_top = visc * (p_even + p_odd) + mass * (w_top * vector(m, n, top))
            q_bottom = visc * (p_even - p_odd) + mass * (w_bottom * vector(m, n, bottom))
            if m + 1 < steps:
                save_block(work, n, top, q_top)
                save_block(work, n, bottom, q_bottom)
            if n == 0:
                for i in range(m + 1):
                    dots_ref[m * (m + 1) // 2 + i] += fold(
                        basis_ref[i, top, :] * q_top + basis_ref[i, bottom, :] * q_bottom
                    )
                at = steps * (steps + 1) // 2 + m
                dots_ref[at] += fold(
                    basis_ref[m, top, :] * own_ref[top, :]
                    + basis_ref[m, bottom, :] * own_ref[bottom, :]
                )

    for m in range(steps):
        if m + 1 == steps:
            apply(m, 0)
            continue
        blocks = (0, 1, 2) if m == 0 else (0, 1)
        for n in blocks:
            apply(m, n)
        tiles = far_tiles if m == 0 else near_tiles
        share_xy(work, tiles)
        share_z(work, tiles)
        outs = (0, 1) if m + 2 < steps else (0,)

        @pl.loop(0, NP)
        def _(k):
            rows = pl.ds(pl.multiple_of(k * FACE, FACE), FACE)
            for n in outs:
                value = (2.0 / bound) * (load_block(inv, n, rows) * load_block(work, n, rows)) - vector(m, n, rows)
                if m > 0:
                    value = value + value - vector(m - 1, n, rows)
                if n == 0:
                    basis_ref[m + 1, rows, :] = value
                else:
                    ghost[m + 1, rows, :] = value

    def plane(load, row):
        total = None
        for k in range(NP):
            term = float(diff[row, k]) * load(k)
            total = term if total is None else total + term
        return total

    lower = lane_masks(FACE)[4]

    def rows_of(k):
        return pl.ds(k * FACE, FACE)

    last = steps - 1
    bottom = plane(lambda k: basis_ref[last, rows_of(k), wide_tile], 0)
    top = plane(lambda k: basis_ref[last, rows_of(k), high_tile], NP - 1)
    message_ref[:FACE] = jnp.where(lower, bottom, top)
    message_ref[FACE:] = jnp.sum(dots_ref[...], axis=1)
    for m in range(steps - 1):
        below = plane(lambda k: ghost[m, rows_of(k), wide_tile], NP - 1)
        above = plane(lambda k: ghost[m, rows_of(k), high_tile], 0)
        near_ref[m] = jnp.where(lower, above, below)


def solve_coefficients(sums):
    size = ITERS
    gram = {}
    for j in range(size):
        for i in range(j + 1):
            at = j * (j + 1) // 2 + i
            gram[j, i] = sums[at : at + 1]
    at = size * (size + 1) // 2
    right = [sums[at + i : at + i + 1] for i in range(size)]
    lower, recip = {}, []
    reduced = {}
    for k in range(size):
        for i in range(k, size):
            value = gram[i, k]
            for m in range(k):
                value = value - lower[i, m] * reduced[k, m]
            reduced[i, k] = value
        pivot = reduced[k, k]
        usable = pivot > 1e-7 * gram[k, k]
        inverse = jnp.where(usable, 1.0 / jnp.where(usable, pivot, 1.0), 0.0)
        recip.append(inverse)
        for i in range(k + 1, size):
            lower[i, k] = reduced[i, k] * inverse
    for k in range(size):
        for m in range(k):
            right[k] = right[k] - lower[k, m] * right[m]
    out = [None] * size
    for k in reversed(range(size)):
        value = right[k] * recip[k]
        for m in range(k + 1, size):
            value = value - lower[m, k] * out[m]
        out[k] = value
    return out


def gradient_kernel(
    diff, sum_a_ref, sum_b_ref, basis_ref, near_ref, fa_ref, fb_ref, dcol_ref,
    grad_ref, vel_ref, work,
):
    elems = basis_ref.shape[2]
    quarters = grad_ref.shape[0]
    quarter = grad_ref.shape[2]
    scalars = jnp.sum(sum_a_ref[...] + sum_b_ref[...], axis=1, keepdims=True)
    part = lax.axis_index("dom")
    parts = lax.axis_size("dom")
    weights = solve_coefficients(scalars)
    tiles = range(elems // TILE)

    @pl.loop(0, NP)
    def _(k):
        rows = pl.ds(pl.multiple_of(k * FACE, FACE), FACE)
        total = weights[0] * basis_ref[0, rows, :]
        for m in range(1, ITERS):
            total = total + weights[m] * basis_ref[m, rows, :]
        vel_ref[rows, :] = total

    lower = lane_masks(FACE)[4]
    x_keep, x_back, y_keep, y_back, _ = lane_masks(FACE)
    odd_part = lax.axis_index("dom") % 2 > 0
    from_above = jnp.where(odd_part, fb_ref[:FACE], fa_ref[:FACE])
    from_below = jnp.where(odd_part, fa_ref[:FACE], fb_ref[:FACE])
    near = weights[ITERS - 1] * jnp.where(lower, from_above, from_below)
    for m in range(ITERS - 1):
        near = near + weights[m] * near_ref[m]
    near = pltpu.roll(near, LAYER, 1)

    def finish(direction, scale):
        share_xy(work, tiles, 0.5)
        if direction == 2:
            first = pl.ds(0, FACE)
            last = pl.ds((NP - 1) * FACE, FACE)
            lows = [work[t, first, :] for t in tiles]
            highs = [work[t, last, :] for t in tiles]
            low_roll = [pltpu.roll(v, LAYER, 1) for v in lows] + [near]
            high_roll = [near] + [pltpu.roll(v, LAYER, 1) for v in highs]
            count = len(tiles)
            for n in tiles:
                up = jnp.where(lower, low_roll[n], low_roll[n + 1])
                down = jnp.where(lower, high_roll[n], high_roll[n + 1])
                high_mean = 0.5 * (highs[n] + up)
                low_mean = 0.5 * (lows[n] + down)
                if n == count - 1:
                    edge = jnp.logical_and(jnp.logical_not(lower), part == parts - 1)
                    high_mean = jnp.where(edge, highs[n], high_mean)
                if n == 0:
                    edge = jnp.logical_and(lower, part == 0)
                    low_mean = jnp.where(edge, lows[n], low_mean)
                work[n, last, :] = high_mean
                work[n, first, :] = low_mean
        for q in range(quarters):
            grad_ref[q, direction] = (load_block(work, 0, pl.ds(q * quarter, quarter)) * scale).astype(BF16)

    @pl.loop(0, NP)
    def _(k):
        rows = pl.ds(pl.multiple_of(k * FACE, FACE), FACE)
        value = vel_ref[rows, :].reshape(NP, NP, elems)
        total = wide(dcol_ref[0], elems)[None] * value
        for shift in range(1, NP):
            total = total + wide(dcol_ref[shift], elems)[None] * pltpu.roll(value, NP - shift, 1)
        save_block(work, 0, rows, total.reshape(FACE, elems))

    finish(0, 1.0 / NP)

    @pl.loop(0, NP)
    def _(k):
        rows = pl.ds(pl.multiple_of(k * FACE, FACE), FACE)
        value = vel_ref[rows, :].reshape(NP, NP, elems)
        for j in range(NP):
            total = float(diff[j, 0]) * value[0]
            for m in range(1, NP):
                total = total + float(diff[j, m]) * value[m]
            save_block(work, 0, pl.ds(pl.multiple_of(k * FACE + j * NP, NP), NP), total)

    finish(1, 1.0 / NP)

    @pl.loop(0, NP)
    def _(j):
        planes = [vel_ref[pl.ds(pl.multiple_of(m * FACE + j * NP, NP), NP), :] for m in range(NP)]
        for k in range(NP):
            total = float(diff[k, 0]) * planes[0]
            for m in range(1, NP):
                total = total + float(diff[k, m]) * planes[m]
            save_block(work, 0, pl.ds(pl.multiple_of(k * FACE + j * NP, NP), NP), total)

    finish(2, 1.0 / NP)


def slots_kernel(order_ref, vel_ref, out_ref):
    elems = order_ref.shape[1]
    cell_by_slot = (iota((elems, elems), 0) == order_ref[...]).astype(F32)
    pick = jnp.transpose(cell_by_slot).astype(BF16)
    high, mid, low = split3(vel_ref[...])
    out_ref[...] = dot_nt(pick, high) + dot_nt(pick, mid) + dot_nt(pick, low)


def middle_eigenvalue(jac):
    strain = [[0.5 * (jac[a][b] + jac[b][a]) for b in range(3)] for a in range(3)]
    spin = [[0.5 * (jac[a][b] - jac[b][a]) for b in range(3)] for a in range(3)]
    mat = [[None] * 3 for _ in range(3)]
    for a in range(3):
        for b in range(a, 3):
            total = strain[a][0] * strain[0][b] + spin[a][0] * spin[0][b]
            for c in (1, 2):
                total = total + strain[a][c] * strain[c][b] + spin[a][c] * spin[c][b]
            mat[a][b] = total
            mat[b][a] = total
    peak = jnp.maximum(jnp.abs(mat[0][1]), jnp.maximum(jnp.abs(mat[0][2]), jnp.abs(mat[1][2])))
    for a in range(3):
        peak = jnp.maximum(peak, jnp.abs(mat[a][a]))
    peak = jnp.where(peak > 0.0, peak, 1.0)
    shrink = 1.0 / peak
    for a in range(3):
        for b in range(a, 3):
            mat[a][b] = mat[b][a] = mat[a][b] * shrink
    for _ in range(SWEEPS):
        for p, q, r in ((0, 1, 2), (0, 2, 1), (1, 2, 0)):
            pivot = mat[p][q]
            first, second = mat[p][p], mat[q][q]
            gap = 0.5 * (first - second)
            norm = pivot * pivot + gap * gap
            inv_norm = lax.rsqrt(jnp.maximum(norm, 1e-37))
            middle = 0.5 * (first + second)
            radius = norm * inv_norm
            turned = norm > 0.0
            cos_two = jnp.where(turned, gap * inv_norm, 1.0)
            half_sin = (0.5 * pivot) * inv_norm
            lead = 0.5 + 0.5 * jnp.abs(cos_two)
            inv_big = lax.rsqrt(lead)
            big = lead * inv_big
            small = half_sin * inv_big
            forward = cos_two >= 0.0
            cosine = jnp.where(forward, big, jnp.abs(small))
            sine = jnp.where(forward, small, jnp.where(pivot < 0.0, -big, big))
            mat[p][p] = middle + radius
            mat[q][q] = middle - radius
            mat[p][q] = mat[q][p] = None
            side_p, side_q = mat[r][p], mat[r][q]
            if side_p is None:
                new_p, new_q = sine * side_q, cosine * side_q
            elif side_q is None:
                new_p, new_q = cosine * side_p, -(sine * side_p)
            else:
                new_p = cosine * side_p + sine * side_q
                new_q = cosine * side_q - sine * side_p
            mat[r][p] = mat[p][r] = new_p
            mat[r][q] = mat[q][r] = new_q
    d0, d1, d2 = mat[0][0], mat[1][1], mat[2][2]
    largest = jnp.maximum(jnp.maximum(d0, d1), d2)
    smallest = jnp.minimum(jnp.minimum(d0, d1), d2)
    return (d0 + d1 + d2 - largest - smallest) * peak


def vortex_kernel(grad_ref, place_ref, out_ref, value):
    rows_all = grad_ref.shape[2]
    step = 16

    @pl.loop(0, rows_all // step)
    def _(n):
        rows = pl.ds(pl.multiple_of(n * step, step), step)
        jac = [[grad_ref[c, d, rows, :].astype(F32) for d in range(3)] for c in range(3)]
        value[rows, :] = middle_eigenvalue(jac)

    high, mid, low = split3(value[...])
    place = place_ref[...]
    moved = dot_nt(place, high) + dot_nt(place, mid) + dot_nt(place, low)
    owners, cap = out_ref.shape[0], out_ref.shape[1]
    used = place.shape[0] // cap
    out_ref[: owners - used] = jnp.zeros((owners - used,) + out_ref.shape[1:], F32)
    out_ref[owners - used :] = moved.reshape((used,) + out_ref.shape[1:])


def final_kernel(vortex_ref, vel_ref, out_ref):
    quarters = vortex_ref.shape[0]
    quarter = vortex_ref.shape[2]

    last = lax.axis_index("grp") == lax.axis_size("grp") - 1

    @pl.when(last)
    def _():
        for q in range(quarters):
            out_ref[0, :, q * quarter : (q + 1) * quarter] = vortex_ref[q]

    @pl.when(jnp.logical_not(last))
    def _():
        out_ref[0] = vel_ref[...]


GRANT = pltpu.CompilerParams(vmem_limit_bytes=24 * 2**20)


def vmem():
    return pl.BlockSpec(memory_space=pltpu.VMEM)


def cost(flops, size):
    return pl.CostEstimate(flops=flops, bytes_accessed=size, transcendentals=0)


def per_device(forcing, viscosity, mass_coef, element_order, owner):
    elems = viscosity.shape[0]
    nodes = forcing.shape[2]
    parts = lax.axis_size("dom")
    groups = lax.axis_size("grp")
    cap = elems // parts
    quarter = nodes // groups
    diff, kmat_np, cols_np, dcol_np, bound = host_tables()
    kmat = jnp.asarray(kmat_np, BF16)
    cols = jnp.asarray(cols_np)
    dcol = jnp.asarray(dcol_np)
    sds = jax.ShapeDtypeStruct

    pack = pl.pallas_call(
        prep_kernel,
        in_specs=[pl.BlockSpec(memory_space=pl.ANY)] + [vmem()] * 4,
        out_specs=vmem(),
        out_shape=sds((nodes + 8, elems), F32),
        scratch_shapes=[pltpu.VMEM((elems, nodes), F32), pltpu.SemaphoreType.DMA],
        cost_estimate=cost(10**9, 2 * 10**6),
        compiler_params=GRANT,
        name="prep",
    )(forcing, element_order, viscosity[None], mass_coef[None], cols)

    swap_a = [(i, i ^ 1) for i in range(parts) if i ^ 1 < parts]
    swap_b = [(i, ((i - 1) ^ 1) + 1) for i in range(1, parts - 1)]
    ghost_a = lax.ppermute(pack, "dom", swap_a)
    ghost_b = lax.ppermute(pack, "dom", swap_b)

    place = pl.pallas_call(
        lambda *refs: place_kernel(cap, *refs),
        in_specs=[vmem(), vmem()],
        out_specs=vmem(),
        out_shape=sds((elems, elems), BF16),
        cost_estimate=cost(10**9, 2 * 10**6),
        compiler_params=GRANT,
        name="place",
    )(element_order, owner)

    basis, near, message = pl.pallas_call(
        lambda *refs: krylov_kernel(diff, bound, *refs),
        in_specs=[vmem()] * 5,
        out_specs=[vmem()] * 3,
        out_shape=[
            sds((ITERS, nodes, elems), F32),
            sds((ITERS - 1, FACE, TILE), F32),
            sds((FACE + 16, TILE), F32),
        ],
        scratch_shapes=[
            pltpu.VMEM((6, nodes, TILE), F32),
            pltpu.VMEM((3, 8, elems), F32),
            pltpu.VMEM((6, nodes, TILE), F32),
            pltpu.VMEM((nodes, elems), F32),
            pltpu.VMEM((ITERS - 1, nodes, elems), F32),
            pltpu.VMEM((2, nodes // 2, elems), BF16),
            pltpu.VMEM((2, nodes // 2, elems), BF16),
            pltpu.VMEM((2, nodes // 2, elems), F32),
            pltpu.VMEM((16, 8, TILE), F32),
        ],
        cost_estimate=cost(10**10, 10**7),
        compiler_params=GRANT,
        name="krylov",
    )(pack, ghost_a, ghost_b, kmat, cols)

    face_a = lax.ppermute(message, "dom", swap_a)
    face_b = lax.ppermute(message, "dom", swap_b)
    pending = (message[FACE:], face_a[FACE:])
    reach = 2
    while reach < parts:
        sums = pending[0] + pending[1]
        pending = (sums, lax.ppermute(sums, "dom", [(i, i ^ reach) for i in range(parts)]))
        reach *= 2

    grads, vel = pl.pallas_call(
        lambda *refs: gradient_kernel(diff, *refs),
        in_specs=[vmem()] * 7,
        out_specs=[vmem()] * 2,
        out_shape=[sds((groups, 3, quarter, elems), BF16), sds((nodes, elems), F32)],
        scratch_shapes=[pltpu.VMEM((2, nodes, TILE), F32)],
        cost_estimate=cost(10**9, 4 * 10**6),
        compiler_params=GRANT,
        name="gradient",
    )(*pending, basis, near, face_a, face_b, dcol)

    exchanged = lax.all_to_all(grads, "grp", split_axis=0, concat_axis=0, tiled=True)

    vel_slot = pl.pallas_call(
        slots_kernel,
        in_specs=[vmem(), vmem()],
        out_specs=vmem(),
        out_shape=sds((elems, nodes), F32),
        cost_estimate=cost(10**9, 2 * 10**6),
        compiler_params=GRANT,
        name="slots",
    )(element_order, vel)

    packed = pl.pallas_call(
        vortex_kernel,
        in_specs=[vmem(), vmem()],
        out_specs=vmem(),
        out_shape=sds((groups * parts, cap, quarter), F32),
        scratch_shapes=[pltpu.VMEM((quarter, elems), F32)],
        cost_estimate=cost(10**9, 2 * 10**6),
        compiler_params=GRANT,
        name="vortex",
    )(exchanged, place)

    received = lax.all_to_all(
        packed, ("grp", "dom"), split_axis=0, concat_axis=0, tiled=True
    )
    return pl.pallas_call(
        final_kernel,
        in_specs=[vmem(), vmem()],
        out_specs=vmem(),
        out_shape=sds((1, elems, nodes), F32),
        cost_estimate=cost(10**6, 2 * 10**6),
        compiler_params=GRANT,
        name="final",
    )(received.reshape(groups, elems, quarter), vel_slot)


def solution(mesh):
    in_specs = (P(None, "dom", None), P("dom"), P("dom"), P("dom", None), P("dom", None))
    out_specs = P("grp", "dom", None)
    return jax.shard_map(
        per_device, mesh=mesh, in_specs=in_specs, out_specs=out_specs, check_vma=False
    )
```

```python
import jax
import jax.numpy as jnp
import numpy as np
from jax import lax
from jax.experimental import pallas as pl
from jax.experimental.pallas import tpu as pltpu
from jax.sharding import PartitionSpec as P

NP = 8
BX = 8
BY = 8
ITERS = 4
SWEEPS = 4
FACE = NP * NP
LAYER = BX * BY
TILE = 2 * LAYER
F32 = jnp.float32
BF16 = jnp.bfloat16


def legendre_values(points, node_count):
    legendre = np.zeros((points.shape[0], node_count))
    legendre[:, 0] = 1.0
    legendre[:, 1] = points
    for poly_order in range(2, node_count):
        legendre[:, poly_order] = (
            (2 * poly_order - 1) * points * legendre[:, poly_order - 1]
            - (poly_order - 1) * legendre[:, poly_order - 2]
        ) / poly_order
    return legendre


def lobatto_table(node_count):
    degree = node_count - 1
    points = np.cos(np.pi * np.arange(node_count) / degree)
    for attempt in range(60):
        legendre = legendre_values(points, node_count)
        points = points - (points * legendre[:, degree] - legendre[:, degree - 1]) / (
            node_count * legendre[:, degree]
        )
    points = points[::-1].copy()
    end_values = legendre_values(points, node_count)[:, degree]
    weights = 2.0 / (degree * node_count * end_values * end_values)
    spacing = points[:, None] - points[None, :] + np.eye(node_count)
    diff_matrix = end_values[:, None] / end_values[None, :] / spacing
    diff_matrix = diff_matrix * (1.0 - np.eye(node_count))
    diff_matrix[0, 0] = -degree * node_count / 4.0
    diff_matrix[-1, -1] = degree * node_count / 4.0
    return (weights, diff_matrix)


def operator_tables(node_count):
    weights, diff_matrix = lobatto_table(node_count)
    identity = np.eye(node_count)
    weight_cube = (
        weights[:, None, None] * weights[None, :, None] * weights[None, None, :]
    ).reshape(-1)
    directional = [
        np.kron(identity, np.kron(identity, diff_matrix)),
        np.kron(identity, np.kron(diff_matrix, identity)),
        np.kron(diff_matrix, np.kron(identity, identity)),
    ]
    stiffness = np.zeros((node_count**3, node_count**3))
    for direction_matrix in directional:
        stiffness = stiffness + direction_matrix.T @ (weight_cube[:, None] * direction_matrix)
    return diff_matrix, weight_cube, stiffness


def split3_np(table):
    parts = []
    rest = np.asarray(table, np.float64)
    for _ in range(3):
        part = rest.astype(np.float32).astype(BF16)
        parts.append(part)
        rest = rest - part.astype(np.float64)
    return parts


def host_tables():
    diff_matrix, weight_cube, stiffness = operator_tables(NP)
    half = FACE * NP // 2
    flip = np.concatenate([np.arange(FACE) + FACE * k for k in range(NP - 1, NP // 2 - 1, -1)])
    top = stiffness[:half, :half]
    cross = stiffness[:half][:, flip]
    even = split3_np(0.5 * (top + cross))
    odd = split3_np(0.5 * (top - cross))
    kmat = np.stack(even + odd)
    diag = np.diag(stiffness)
    scaled = stiffness / np.sqrt(diag[:, None] * diag[None, :])
    bound = max(1.0, float(np.linalg.eigvalsh(scaled)[-1]))
    cols = np.stack([weight_cube, diag]).astype(np.float32)
    cols = np.ascontiguousarray(np.broadcast_to(cols[:, :, None], cols.shape + (TILE,)))
    dcol = np.zeros((NP, NP, TILE), np.float32)
    for shift in range(NP):
        for row in range(NP):
            dcol[shift, row] = diff_matrix[row, (row + shift) % NP]
    return diff_matrix, kmat, cols, dcol, bound


def split3(value):
    high = value.astype(BF16)
    rest = value - high.astype(F32)
    mid = rest.astype(BF16)
    low = (rest - mid.astype(F32)).astype(BF16)
    return high, mid, low


def dot_nn(a, b):
    return jnp.dot(a, b, preferred_element_type=F32)


def dot_nt(a, b):
    return lax.dot_general(a, b, (((1,), (1,)), ((), ())), preferred_element_type=F32)


def iota(shape, dim):
    return lax.broadcasted_iota(jnp.int32, shape, dim)


def wide(col, lanes):
    return jnp.concatenate([col] * (lanes // col.shape[1]), axis=1)


def prep_kernel(
    force_hbm, order_hbm, visc_hbm, mass_hbm, cols_hbm, pack_ref,
    force_ref, order_ref, visc_ref, mass_ref, cols_ref, sem,
):
    elems = order_ref.shape[1]
    nodes = force_ref.shape[1]
    component = jnp.minimum(lax.axis_index("grp"), 2)
    copies = [
        pltpu.make_async_copy(order_hbm, order_ref, sem.at[0]),
        pltpu.make_async_copy(visc_hbm, visc_ref, sem.at[1]),
        pltpu.make_async_copy(mass_hbm, mass_ref, sem.at[2]),
        pltpu.make_async_copy(force_hbm.at[component], force_ref, sem.at[3]),
        pltpu.make_async_copy(cols_hbm.at[0], cols_ref, sem.at[4]),
    ]
    for copy in copies:
        copy.start()
    for copy in copies[:3]:
        copy.wait()
    cell_by_slot = (iota((elems, elems), 0) == order_ref[...]).astype(F32)
    perm = jnp.transpose(cell_by_slot).astype(BF16)
    coef = jnp.concatenate([visc_ref[...], mass_ref[...], jnp.zeros((6, elems), F32)], axis=0)
    high, mid, low = split3(coef)
    coef = dot_nn(high, perm) + dot_nn(mid, perm) + dot_nn(low, perm)
    pack_ref[nodes:, :] = coef
    for copy in copies[3:]:
        copy.wait()
    chunk = 128
    for at in range(0, nodes, chunk):
        piece = jnp.transpose(force_ref[:, at : at + chunk])
        high, mid, low = split3(piece)
        moved = dot_nn(high, perm) + dot_nn(mid, perm) + dot_nn(low, perm)
        moved = wide(cols_ref[at : at + chunk, :], elems) * moved
        pack_ref[at : at + chunk, :] = moved


def place_kernel(cap, order_ref, owner_ref, place_ref):
    elems = order_ref.shape[1]
    owners = elems // cap
    rows = max(8, owners)
    owner_row = owner_ref[...]
    match = (iota((rows, elems), 0) == owner_row).astype(F32)
    before = (iota((elems, elems), 0) < iota((elems, elems), 1)).astype(BF16)
    running = dot_nn(match.astype(BF16), before)
    rank = jnp.sum(match * running, axis=0, keepdims=True).astype(jnp.int32)
    dest = jnp.where(owner_row >= 0, owner_row * cap + rank, -1)
    to_dest = (iota((elems, elems), 0) == dest).astype(BF16)
    cell_by_slot = (iota((elems, elems), 0) == order_ref[...]).astype(BF16)
    place_ref[...] = dot_nt(to_dest, cell_by_slot).astype(BF16)


def lane_masks(rows):
    lane = iota((rows, TILE), 1)
    x_pos = lane % BX
    y_pos = lane // BX % BY
    return x_pos < BX - 1, x_pos > 0, y_pos < BY - 1, y_pos > 0, lane < LAYER


def pair(first, second, keep, back, stride, scale):
    up = pltpu.roll(first, TILE - stride, 1)
    down = pltpu.roll(second, stride, 1)
    if scale is None:
        return first + jnp.where(back, down, 0.0), second + jnp.where(keep, up, 0.0)
    return (
        jnp.where(back, scale * (first + down), first),
        jnp.where(keep, scale * (second + up), second),
    )


def share_xy(ref, tiles, scale=None):
    x_keep, x_back, y_keep, y_back, _ = lane_masks(FACE)
    y_keep, y_back = y_keep[:NP], y_back[:NP]
    for t in tiles:
        low = ref[t, pl.ds(0, FACE, stride=NP), :]
        high = ref[t, pl.ds(NP - 1, FACE, stride=NP), :]
        low, high = pair(low, high, x_keep, x_back, 1, scale)
        ref[t, pl.ds(0, FACE, stride=NP), :] = low
        ref[t, pl.ds(NP - 1, FACE, stride=NP), :] = high
        for k in range(NP):
            first = pl.ds(k * FACE, NP)
            last = pl.ds(k * FACE + FACE - NP, NP)
            low, high = pair(ref[t, first, :], ref[t, last, :], y_keep, y_back, BX, scale)
            ref[t, first, :] = low
            ref[t, last, :] = high


def load_block(ref, n, rows):
    return jnp.concatenate([ref[2 * n, rows, :], ref[2 * n + 1, rows, :]], axis=1)


def save_block(ref, n, rows, value):
    ref[2 * n, rows, :] = value[:, :TILE]
    ref[2 * n + 1, rows, :] = value[:, TILE:]


def share_z(ref, tiles):
    lower = lane_masks(FACE)[4]
    first = pl.ds(0, FACE)
    last = pl.ds((NP - 1) * FACE, FACE)
    lows = [ref[t, first, :] for t in tiles]
    highs = [ref[t, last, :] for t in tiles]
    low_roll = [pltpu.roll(v, LAYER, 1) for v in lows] + [jnp.zeros((FACE, TILE), F32)]
    high_roll = [jnp.zeros((FACE, TILE), F32)] + [pltpu.roll(v, LAYER, 1) for v in highs]
    for n, t in enumerate(tiles):
        up = jnp.where(lower, low_roll[n], low_roll[n + 1])
        down = jnp.where(lower, high_roll[n], high_roll[n + 1])
        ref[t, last, :] = highs[n] + up
        ref[t, first, :] = lows[n] + down


def stage_kernel(own_ref, cols_ref, raw_ref, rhs_ref, jac_ref):
    nodes = cols_ref.shape[1]
    elems = own_ref.shape[1]
    raw_ref[nodes:, :] = own_ref[nodes:, :]

    @pl.loop(0, NP)
    def _(k):
        rows = pl.ds(pl.multiple_of(k * FACE, FACE), FACE)
        value = own_ref[rows, :]
        raw_ref[rows, :] = value
        save_block(rhs_ref, 0, rows, value)
        w_col = wide(cols_ref[0, rows, :], elems)
        d_col = wide(cols_ref[1, rows, :], elems)
        visc = own_ref[nodes : nodes + 1, :]
        mass = own_ref[nodes + 1 : nodes + 2, :]
        save_block(jac_ref, 0, rows, visc * d_col + mass * w_col)

    share_xy(rhs_ref, [0, 1])
    share_xy(jac_ref, [0, 1])


def krylov_kernel(
    diff, bound, own_ref, rhs_ref, jac_ref, a_ref, b_ref, kmat_ref, cols_ref,
    basis_ref, near_ref, message_ref,
    work, coef, inv, vec, ghost, even, odd, prod, dots_ref,
):
    nodes = cols_ref.shape[1]
    elems = own_ref.shape[1]
    half = nodes // 2
    steps = ITERS
    odd_part = lax.axis_index("dom") % 2 > 0
    wide_tile = pl.ds(0, TILE)
    high_tile = pl.ds(TILE, TILE)

    def gather(rows, out_near, out_far):
        a_low, a_high = a_ref[rows, wide_tile], a_ref[rows, high_tile]
        b_low, b_high = b_ref[rows, wide_tile], b_ref[rows, high_tile]
        out_near(
            jnp.where(odd_part, a_high, b_high), jnp.where(odd_part, b_low, a_low)
        )
        out_far(
            jnp.where(odd_part, a_low, b_low), jnp.where(odd_part, b_high, a_high)
        )

    def store(ref, n, rows):
        def put(*parts):
            save_block(ref, n, rows, parts[0] if len(parts) == 1 else jnp.concatenate(parts, axis=1))
        return put

    def store_coef(n):
        def put(*parts):
            coef[n] = parts[0] if len(parts) == 1 else jnp.concatenate(parts, axis=1)
        return put

    tail = pl.ds(nodes, own_ref.shape[0] - nodes)
    coef[0] = own_ref[tail, :]
    gather(tail, store_coef(1), store_coef(2))

    @pl.loop(0, NP)
    def _(k):
        rows = pl.ds(pl.multiple_of(k * FACE, FACE), FACE)
        gather(rows, store(work, 1, rows), store(work, 2, rows))
        for t in range(2):
            work[t, rows, :] = rhs_ref[t, rows, :]
            inv[t, rows, :] = jac_ref[t, rows, :]
        w_col = wide(cols_ref[0, rows, :], elems)
        d_col = wide(cols_ref[1, rows, :], elems)
        for n in range(1, 3):
            save_block(inv, n, rows, coef[n, 0:1, :] * d_col + coef[n, 1:2, :] * w_col)

    far_tiles = [4, 2, 0, 1, 3, 5]
    near_tiles = far_tiles[1:5]
    share_xy(work, [2, 3, 4, 5])
    share_z(work, far_tiles)
    share_xy(inv, [2, 3, 4, 5])
    share_z(inv, far_tiles)

    @pl.loop(0, NP)
    def _(k):
        rows = pl.ds(pl.multiple_of(k * FACE, FACE), FACE)
        for n in range(3):
            total = load_block(inv, n, rows)
            recip = jnp.where(total > 0.0, 1.0 / total, 0.0)
            save_block(inv, n, rows, recip)
            value = recip * load_block(work, n, rows)
            if n == 0:
                basis_ref[0, rows, :] = value
            elif n == 1:
                ghost[0, rows, :] = value
            else:
                vec[rows, :] = value

    def vector(m, n, rows):
        if n == 0:
            return basis_ref[m, rows, :]
        return ghost[m, rows, :] if n == 1 else vec[rows, :]

    dots_ref[...] = jnp.zeros_like(dots_ref)

    def fold(value):
        rows, lanes = value.shape
        total = jnp.sum(value.reshape(rows // 8, 8, lanes), axis=0)
        return sum(total[:, at : at + TILE] for at in range(0, lanes, TILE))

    def apply(m, n):
        @pl.loop(0, NP // 2)
        def _(k):
            top = pl.ds(pl.multiple_of(k * FACE, FACE), FACE)
            bottom = pl.ds(pl.multiple_of((NP - 1 - k) * FACE, FACE), FACE)
            v_top = vector(m, n, top)
            v_bottom = vector(m, n, bottom)
            for part, ref in ((v_top + v_bottom, even), (v_top - v_bottom, odd)):
                high = part.astype(BF16)
                ref[0, top, :] = high
                ref[1, top, :] = (part - high.astype(F32)).astype(BF16)

        for parity, ref in ((0, even), (1, odd)):
            base = 3 * parity
            prod[parity] = (
                dot_nn(kmat_ref[base + 1], ref[1])
                + dot_nn(kmat_ref[base + 2], ref[0])
                + dot_nn(kmat_ref[base], ref[1])
                + dot_nn(kmat_ref[base + 1], ref[0])
                + dot_nn(kmat_ref[base], ref[0])
            )

        @pl.loop(0, NP // 2)
        def _(k):
            top = pl.ds(pl.multiple_of(k * FACE, FACE), FACE)
            bottom = pl.ds(pl.multiple_of((NP - 1 - k) * FACE, FACE), FACE)
            p_even = prod[0, top, :]
            p_odd = prod[1, top, :]
            w_top = wide(cols_ref[0, top, :], elems)
            w_bottom = wide(cols_ref[0, bottom, :], elems)
            visc = coef[n, 0:1, :]
            mass = coef[n, 1:2, :]
            q_top = visc * (p_even + p_odd) + mass * (w_top * vector(m, n, top))
            q_bottom = visc * (p_even - p_odd) + mass * (w_bottom * vector(m, n, bottom))
            if m + 1 < steps:
                save_block(work, n, top, q_top)
                save_block(work, n, bottom, q_bottom)
            if n == 0:
                for i in range(m + 1):
                    dots_ref[m * (m + 1) // 2 + i] += fold(
                        basis_ref[i, top, :] * q_top + basis_ref[i, bottom, :] * q_bottom
                    )
                at = steps * (steps + 1) // 2 + m
                dots_ref[at] += fold(
                    basis_ref[m, top, :] * own_ref[top, :]
                    + basis_ref[m, bottom, :] * own_ref[bottom, :]
                )

    for m in range(steps):
        if m + 1 == steps:
            apply(m, 0)
            continue
        blocks = (0, 1, 2) if m == 0 else (0, 1)
        for n in blocks:
            apply(m, n)
        tiles = far_tiles if m == 0 else near_tiles
        share_xy(work, tiles)
        share_z(work, tiles)
        outs = (0, 1) if m + 2 < steps else (0,)

        @pl.loop(0, NP)
        def _(k):
            rows = pl.ds(pl.multiple_of(k * FACE, FACE), FACE)
            for n in outs:
                value = (2.0 / bound) * (load_block(inv, n, rows) * load_block(work, n, rows)) - vector(m, n, rows)
                if m > 0:
                    value = value + value - vector(m - 1, n, rows)
                if n == 0:
                    basis_ref[m + 1, rows, :] = value
                else:
                    ghost[m + 1, rows, :] = value

    def plane(load, row):
        total = None
        for k in range(NP):
            term = float(diff[row, k]) * load(k)
            total = term if total is None else total + term
        return total

    lower = lane_masks(FACE)[4]

    def rows_of(k):
        return pl.ds(k * FACE, FACE)

    last = steps - 1
    bottom = plane(lambda k: basis_ref[last, rows_of(k), wide_tile], 0)
    top = plane(lambda k: basis_ref[last, rows_of(k), high_tile], NP - 1)
    message_ref[:FACE] = jnp.where(lower, bottom, top)
    message_ref[FACE:] = jnp.sum(dots_ref[...], axis=1)
    for m in range(steps - 1):
        below = plane(lambda k: ghost[m, rows_of(k), wide_tile], NP - 1)
        above = plane(lambda k: ghost[m, rows_of(k), high_tile], 0)
        near_ref[m] = jnp.where(lower, above, below)


def solve_coefficients(sums):
    size = ITERS
    gram = {}
    for j in range(size):
        for i in range(j + 1):
            at = j * (j + 1) // 2 + i
            gram[j, i] = sums[at : at + 1]
    at = size * (size + 1) // 2
    right = [sums[at + i : at + i + 1] for i in range(size)]
    lower, recip = {}, []
    reduced = {}
    for k in range(size):
        for i in range(k, size):
            value = gram[i, k]
            for m in range(k):
                value = value - lower[i, m] * reduced[k, m]
            reduced[i, k] = value
        pivot = reduced[k, k]
        usable = pivot > 1e-7 * gram[k, k]
        inverse = jnp.where(usable, 1.0 / jnp.where(usable, pivot, 1.0), 0.0)
        recip.append(inverse)
        for i in range(k + 1, size):
            lower[i, k] = reduced[i, k] * inverse
    for k in range(size):
        for m in range(k):
            right[k] = right[k] - lower[k, m] * right[m]
    out = [None] * size
    for k in reversed(range(size)):
        value = right[k] * recip[k]
        for m in range(k + 1, size):
            value = value - lower[m, k] * out[m]
        out[k] = value
    return out


def gradient_kernel(
    diff, sum_a_ref, sum_b_ref, basis_ref, near_ref, fa_ref, fb_ref, dcol_ref,
    grad_ref, vel_ref, work,
):
    elems = basis_ref.shape[2]
    quarters = grad_ref.shape[0]
    quarter = grad_ref.shape[2]
    scalars = jnp.sum(sum_a_ref[...] + sum_b_ref[...], axis=1, keepdims=True)
    part = lax.axis_index("dom")
    parts = lax.axis_size("dom")
    weights = solve_coefficients(scalars)
    tiles = range(elems // TILE)

    @pl.loop(0, NP)
    def _(k):
        rows = pl.ds(pl.multiple_of(k * FACE, FACE), FACE)
        total = weights[0] * basis_ref[0, rows, :]
        for m in range(1, ITERS):
            total = total + weights[m] * basis_ref[m, rows, :]
        vel_ref[rows, :] = total

    lower = lane_masks(FACE)[4]
    x_keep, x_back, y_keep, y_back, _ = lane_masks(FACE)
    odd_part = lax.axis_index("dom") % 2 > 0
    from_above = jnp.where(odd_part, fb_ref[:FACE], fa_ref[:FACE])
    from_below = jnp.where(odd_part, fa_ref[:FACE], fb_ref[:FACE])
    near = weights[ITERS - 1] * jnp.where(lower, from_above, from_below)
    for m in range(ITERS - 1):
        near = near + weights[m] * near_ref[m]
    near = pltpu.roll(near, LAYER, 1)

    def finish(direction, scale):
        share_xy(work, tiles, 0.5)
        if direction == 2:
            first = pl.ds(0, FACE)
            last = pl.ds((NP - 1) * FACE, FACE)
            lows = [work[t, first, :] for t in tiles]
            highs = [work[t, last, :] for t in tiles]
            low_roll = [pltpu.roll(v, LAYER, 1) for v in lows] + [near]
            high_roll = [near] + [pltpu.roll(v, LAYER, 1) for v in highs]
            count = len(tiles)
            for n in tiles:
                up = jnp.where(lower, low_roll[n], low_roll[n + 1])
                down = jnp.where(lower, high_roll[n], high_roll[n + 1])
                high_mean = 0.5 * (highs[n] + up)
                low_mean = 0.5 * (lows[n] + down)
                if n == count - 1:
                    edge = jnp.logical_and(jnp.logical_not(lower), part == parts - 1)
                    high_mean = jnp.where(edge, highs[n], high_mean)
                if n == 0:
                    edge = jnp.logical_and(lower, part == 0)
                    low_mean = jnp.where(edge, lows[n], low_mean)
                work[n, last, :] = high_mean
                work[n, first, :] = low_mean
        for q in range(quarters):
            grad_ref[q, direction] = (load_block(work, 0, pl.ds(q * quarter, quarter)) * scale).astype(BF16)

    @pl.loop(0, NP)
    def _(k):
        rows = pl.ds(pl.multiple_of(k * FACE, FACE), FACE)
        value = vel_ref[rows, :].reshape(NP, NP, elems)
        total = wide(dcol_ref[0], elems)[None] * value
        for shift in range(1, NP):
            total = total + wide(dcol_ref[shift], elems)[None] * pltpu.roll(value, NP - shift, 1)
        save_block(work, 0, rows, total.reshape(FACE, elems))

    finish(0, 1.0 / NP)

    @pl.loop(0, NP)
    def _(k):
        rows = pl.ds(pl.multiple_of(k * FACE, FACE), FACE)
        value = vel_ref[rows, :].reshape(NP, NP, elems)
        for j in range(NP):
            total = float(diff[j, 0]) * value[0]
            for m in range(1, NP):
                total = total + float(diff[j, m]) * value[m]
            save_block(work, 0, pl.ds(pl.multiple_of(k * FACE + j * NP, NP), NP), total)

    finish(1, 1.0 / NP)

    @pl.loop(0, NP)
    def _(j):
        planes = [vel_ref[pl.ds(pl.multiple_of(m * FACE + j * NP, NP), NP), :] for m in range(NP)]
        for k in range(NP):
            total = float(diff[k, 0]) * planes[0]
            for m in range(1, NP):
                total = total + float(diff[k, m]) * planes[m]
            save_block(work, 0, pl.ds(pl.multiple_of(k * FACE + j * NP, NP), NP), total)

    finish(2, 1.0 / NP)


def slots_kernel(order_ref, vel_ref, out_ref):
    elems = order_ref.shape[1]
    cell_by_slot = (iota((elems, elems), 0) == order_ref[...]).astype(F32)
    pick = jnp.transpose(cell_by_slot).astype(BF16)
    high, mid, low = split3(vel_ref[...])
    out_ref[...] = dot_nt(pick, high) + dot_nt(pick, mid) + dot_nt(pick, low)


def middle_eigenvalue(jac):
    strain = [[0.5 * (jac[a][b] + jac[b][a]) for b in range(3)] for a in range(3)]
    spin = [[0.5 * (jac[a][b] - jac[b][a]) for b in range(3)] for a in range(3)]
    mat = [[None] * 3 for _ in range(3)]
    for a in range(3):
        for b in range(a, 3):
            total = strain[a][0] * strain[0][b] + spin[a][0] * spin[0][b]
            for c in (1, 2):
                total = total + strain[a][c] * strain[c][b] + spin[a][c] * spin[c][b]
            mat[a][b] = total
            mat[b][a] = total
    peak = jnp.maximum(jnp.abs(mat[0][1]), jnp.maximum(jnp.abs(mat[0][2]), jnp.abs(mat[1][2])))
    for a in range(3):
        peak = jnp.maximum(peak, jnp.abs(mat[a][a]))
    peak = jnp.where(peak > 0.0, peak, 1.0)
    shrink = 1.0 / peak
    for a in range(3):
        for b in range(a, 3):
            mat[a][b] = mat[b][a] = mat[a][b] * shrink
    for _ in range(SWEEPS):
        for p, q, r in ((0, 1, 2), (0, 2, 1), (1, 2, 0)):
            pivot = mat[p][q]
            first, second = mat[p][p], mat[q][q]
            gap = 0.5 * (first - second)
            norm = pivot * pivot + gap * gap
            inv_norm = lax.rsqrt(jnp.maximum(norm, 1e-37))
            middle = 0.5 * (first + second)
            radius = norm * inv_norm
            turned = norm > 0.0
            cos_two = jnp.where(turned, gap * inv_norm, 1.0)
            half_sin = (0.5 * pivot) * inv_norm
            lead = 0.5 + 0.5 * jnp.abs(cos_two)
            inv_big = lax.rsqrt(lead)
            big = lead * inv_big
            small = half_sin * inv_big
            forward = cos_two >= 0.0
            cosine = jnp.where(forward, big, jnp.abs(small))
            sine = jnp.where(forward, small, jnp.where(pivot < 0.0, -big, big))
            mat[p][p] = middle + radius
            mat[q][q] = middle - radius
            mat[p][q] = mat[q][p] = None
            side_p, side_q = mat[r][p], mat[r][q]
            if side_p is None:
                new_p, new_q = sine * side_q, cosine * side_q
            elif side_q is None:
                new_p, new_q = cosine * side_p, -(sine * side_p)
            else:
                new_p = cosine * side_p + sine * side_q
                new_q = cosine * side_q - sine * side_p
            mat[r][p] = mat[p][r] = new_p
            mat[r][q] = mat[q][r] = new_q
    d0, d1, d2 = mat[0][0], mat[1][1], mat[2][2]
    largest = jnp.maximum(jnp.maximum(d0, d1), d2)
    smallest = jnp.minimum(jnp.minimum(d0, d1), d2)
    return (d0 + d1 + d2 - largest - smallest) * peak


def vortex_kernel(grad_ref, place_ref, out_ref, value):
    rows_all = grad_ref.shape[2]
    step = 16

    @pl.loop(0, rows_all // step)
    def _(n):
        rows = pl.ds(pl.multiple_of(n * step, step), step)
        jac = [[grad_ref[c, d, rows, :].astype(F32) for d in range(3)] for c in range(3)]
        value[rows, :] = middle_eigenvalue(jac)

    high, mid, low = split3(value[...])
    place = place_ref[...]
    moved = dot_nt(place, high) + dot_nt(place, mid) + dot_nt(place, low)
    owners, cap = out_ref.shape[0], out_ref.shape[1]
    used = place.shape[0] // cap
    out_ref[: owners - used] = jnp.zeros((owners - used,) + out_ref.shape[1:], F32)
    out_ref[owners - used :] = moved.reshape((used,) + out_ref.shape[1:])


def final_kernel(vortex_ref, vel_ref, out_ref):
    quarters = vortex_ref.shape[0]
    quarter = vortex_ref.shape[2]

    last = lax.axis_index("grp") == lax.axis_size("grp") - 1

    @pl.when(last)
    def _():
        for q in range(quarters):
            out_ref[0, :, q * quarter : (q + 1) * quarter] = vortex_ref[q]

    @pl.when(jnp.logical_not(last))
    def _():
        out_ref[0] = vel_ref[...]


PREP_LIMIT = 67043328 - 2600 * 1024
GRANT = pltpu.CompilerParams(vmem_limit_bytes=24 * 2**20)


def vmem():
    return pl.BlockSpec(memory_space=pltpu.VMEM)


def cost(flops, size):
    return pl.CostEstimate(flops=flops, bytes_accessed=size, transcendentals=0)


def per_device(forcing, viscosity, mass_coef, element_order, owner):
    elems = viscosity.shape[0]
    nodes = forcing.shape[2]
    parts = lax.axis_size("dom")
    groups = lax.axis_size("grp")
    cap = elems // parts
    quarter = nodes // groups
    diff, kmat_np, cols_np, dcol_np, bound = host_tables()
    kmat = jnp.asarray(kmat_np, BF16)
    cols = jnp.asarray(cols_np)
    dcol = jnp.asarray(dcol_np)
    sds = jax.ShapeDtypeStruct

    pack = pl.pallas_call(
        prep_kernel,
        in_specs=[pl.BlockSpec(memory_space=pltpu.HBM)] * 5,
        out_specs=vmem(),
        out_shape=sds((nodes + 8, elems), F32),
        scratch_shapes=[
            pltpu.VMEM((elems, nodes), F32),
            pltpu.VMEM((1, elems), jnp.int32),
            pltpu.VMEM((1, elems), F32),
            pltpu.VMEM((1, elems), F32),
            pltpu.VMEM((nodes, TILE), F32),
            pltpu.SemaphoreType.DMA((5,)),
        ],
        cost_estimate=cost(10**9, 2 * 10**6),
        compiler_params=pltpu.CompilerParams(vmem_limit_bytes=PREP_LIMIT),
        name="prep",
    )(forcing, element_order, viscosity[None], mass_coef[None], cols)

    swap_a = [(i, i ^ 1) for i in range(parts) if i ^ 1 < parts]
    swap_b = [(i, ((i - 1) ^ 1) + 1) for i in range(1, parts - 1)]
    ghost_b = lax.ppermute(pack, "dom", swap_b)
    ghost_a = lax.ppermute(pack, "dom", swap_a)

    raw, rhs_xy, jac_xy = pl.pallas_call(
        stage_kernel,
        in_specs=[vmem()] * 2,
        out_specs=[vmem()] * 3,
        out_shape=[
            sds((nodes + 8, elems), F32),
            sds((2, nodes, TILE), F32),
            sds((2, nodes, TILE), F32),
        ],
        cost_estimate=cost(10**9, 2 * 10**6),
        compiler_params=GRANT,
        name="stage",
    )(pack, cols)

    place = pl.pallas_call(
        lambda *refs: place_kernel(cap, *refs),
        in_specs=[vmem(), vmem()],
        out_specs=vmem(),
        out_shape=sds((elems, elems), BF16),
        cost_estimate=cost(10**9, 2 * 10**6),
        compiler_params=GRANT,
        name="place",
    )(element_order, owner)

    basis, near, message = pl.pallas_call(
        lambda *refs: krylov_kernel(diff, bound, *refs),
        in_specs=[vmem()] * 7,
        out_specs=[vmem()] * 3,
        out_shape=[
            sds((ITERS, nodes, elems), F32),
            sds((ITERS - 1, FACE, TILE), F32),
            sds((FACE + 16, TILE), F32),
        ],
        scratch_shapes=[
            pltpu.VMEM((6, nodes, TILE), F32),
            pltpu.VMEM((3, 8, elems), F32),
            pltpu.VMEM((6, nodes, TILE), F32),
            pltpu.VMEM((nodes, elems), F32),
            pltpu.VMEM((ITERS - 1, nodes, elems), F32),
            pltpu.VMEM((2, nodes // 2, elems), BF16),
            pltpu.VMEM((2, nodes // 2, elems), BF16),
            pltpu.VMEM((2, nodes // 2, elems), F32),
            pltpu.VMEM((16, 8, TILE), F32),
        ],
        cost_estimate=cost(10**10, 10**7),
        compiler_params=GRANT,
        name="krylov",
    )(raw, rhs_xy, jac_xy, ghost_a, ghost_b, kmat, cols)

    face_a = lax.ppermute(message, "dom", swap_a)
    face_b = lax.ppermute(message, "dom", swap_b)
    pending = (message[FACE:], face_a[FACE:])
    reach = 2
    while reach < parts:
        sums = pending[0] + pending[1]
        pending = (sums, lax.ppermute(sums, "dom", [(i, i ^ reach) for i in range(parts)]))
        reach *= 2

    grads, vel = pl.pallas_call(
        lambda *refs: gradient_kernel(diff, *refs),
        in_specs=[vmem()] * 7,
        out_specs=[vmem()] * 2,
        out_shape=[sds((groups, 3, quarter, elems), BF16), sds((nodes, elems), F32)],
        scratch_shapes=[pltpu.VMEM((2, nodes, TILE), F32)],
        cost_estimate=cost(10**9, 4 * 10**6),
        compiler_params=GRANT,
        name="gradient",
    )(*pending, basis, near, face_a, face_b, dcol)

    exchanged = lax.all_to_all(grads, "grp", split_axis=0, concat_axis=0, tiled=True)

    vel_slot = pl.pallas_call(
        slots_kernel,
        in_specs=[vmem(), vmem()],
        out_specs=vmem(),
        out_shape=sds((elems, nodes), F32),
        cost_estimate=cost(10**9, 2 * 10**6),
        compiler_params=GRANT,
        name="slots",
    )(element_order, vel)

    packed = pl.pallas_call(
        vortex_kernel,
        in_specs=[vmem(), vmem()],
        out_specs=vmem(),
        out_shape=sds((groups * parts, cap, quarter), F32),
        scratch_shapes=[pltpu.VMEM((quarter, elems), F32)],
        cost_estimate=cost(10**9, 2 * 10**6),
        compiler_params=GRANT,
        name="vortex",
    )(exchanged, place)

    received = lax.all_to_all(
        packed, ("grp", "dom"), split_axis=0, concat_axis=0, tiled=True
    )
    return pl.pallas_call(
        final_kernel,
        in_specs=[vmem(), vmem()],
        out_specs=vmem(),
        out_shape=sds((1, elems, nodes), F32),
        cost_estimate=cost(10**6, 2 * 10**6),
        compiler_params=GRANT,
        name="final",
    )(received.reshape(groups, elems, quarter), vel_slot)


def solution(mesh):
    in_specs = (P(None, "dom", None), P("dom"), P("dom"), P("dom", None), P("dom", None))
    out_specs = P("grp", "dom", None)
    return jax.shard_map(
        per_device, mesh=mesh, in_specs=in_specs, out_specs=out_specs, check_vma=False
    )
```

```python
import jax
import jax.numpy as jnp
import numpy as np
from jax import lax
from jax.experimental import pallas as pl
from jax.experimental.pallas import tpu as pltpu
from jax.sharding import PartitionSpec as P

NP = 8
BX = 8
BY = 8
ITERS = 4
SWEEPS = 4
FACE = NP * NP
LAYER = BX * BY
TILE = 2 * LAYER
F32 = jnp.float32
BF16 = jnp.bfloat16


def legendre_values(points, node_count):
    legendre = np.zeros((points.shape[0], node_count))
    legendre[:, 0] = 1.0
    legendre[:, 1] = points
    for poly_order in range(2, node_count):
        legendre[:, poly_order] = (
            (2 * poly_order - 1) * points * legendre[:, poly_order - 1]
            - (poly_order - 1) * legendre[:, poly_order - 2]
        ) / poly_order
    return legendre


def lobatto_table(node_count):
    degree = node_count - 1
    points = np.cos(np.pi * np.arange(node_count) / degree)
    for attempt in range(60):
        legendre = legendre_values(points, node_count)
        points = points - (points * legendre[:, degree] - legendre[:, degree - 1]) / (
            node_count * legendre[:, degree]
        )
    points = points[::-1].copy()
    end_values = legendre_values(points, node_count)[:, degree]
    weights = 2.0 / (degree * node_count * end_values * end_values)
    spacing = points[:, None] - points[None, :] + np.eye(node_count)
    diff_matrix = end_values[:, None] / end_values[None, :] / spacing
    diff_matrix = diff_matrix * (1.0 - np.eye(node_count))
    diff_matrix[0, 0] = -degree * node_count / 4.0
    diff_matrix[-1, -1] = degree * node_count / 4.0
    return (weights, diff_matrix)


def operator_tables(node_count):
    weights, diff_matrix = lobatto_table(node_count)
    identity = np.eye(node_count)
    weight_cube = (
        weights[:, None, None] * weights[None, :, None] * weights[None, None, :]
    ).reshape(-1)
    directional = [
        np.kron(identity, np.kron(identity, diff_matrix)),
        np.kron(identity, np.kron(diff_matrix, identity)),
        np.kron(diff_matrix, np.kron(identity, identity)),
    ]
    stiffness = np.zeros((node_count**3, node_count**3))
    for direction_matrix in directional:
        stiffness = stiffness + direction_matrix.T @ (weight_cube[:, None] * direction_matrix)
    return diff_matrix, weight_cube, stiffness


def split3_np(table):
    parts = []
    rest = np.asarray(table, np.float64)
    for _ in range(3):
        part = rest.astype(np.float32).astype(BF16)
        parts.append(part)
        rest = rest - part.astype(np.float64)
    return parts


def host_tables():
    diff_matrix, weight_cube, stiffness = operator_tables(NP)
    half = FACE * NP // 2
    flip = np.concatenate([np.arange(FACE) + FACE * k for k in range(NP - 1, NP // 2 - 1, -1)])
    top = stiffness[:half, :half]
    cross = stiffness[:half][:, flip]
    even = split3_np(0.5 * (top + cross))
    odd = split3_np(0.5 * (top - cross))
    kmat = np.stack(even + odd)
    diag = np.diag(stiffness)
    scaled = stiffness / np.sqrt(diag[:, None] * diag[None, :])
    bound = max(1.0, float(np.linalg.eigvalsh(scaled)[-1]))
    cols = np.stack([weight_cube, diag]).astype(np.float32)
    cols = np.ascontiguousarray(np.broadcast_to(cols[:, :, None], cols.shape + (TILE,)))
    dcol = np.zeros((NP, NP, TILE), np.float32)
    for shift in range(NP):
        for row in range(NP):
            dcol[shift, row] = diff_matrix[row, (row + shift) % NP]
    return diff_matrix, kmat, cols, dcol, bound


def split3(value):
    high = value.astype(BF16)
    rest = value - high.astype(F32)
    mid = rest.astype(BF16)
    low = (rest - mid.astype(F32)).astype(BF16)
    return high, mid, low


def dot_nn(a, b):
    return jnp.dot(a, b, preferred_element_type=F32)


def dot_nt(a, b):
    return lax.dot_general(a, b, (((1,), (1,)), ((), ())), preferred_element_type=F32)


def iota(shape, dim):
    return lax.broadcasted_iota(jnp.int32, shape, dim)


def wide(col, lanes):
    return jnp.concatenate([col] * (lanes // col.shape[1]), axis=1)


def prep_kernel(
    force_hbm, order_hbm, visc_hbm, mass_hbm, cols_hbm, pack_ref,
    force_ref, order_ref, visc_ref, mass_ref, cols_ref, sem,
):
    elems = order_ref.shape[1]
    nodes = force_ref.shape[1]
    component = jnp.minimum(lax.axis_index("grp"), 2)
    copies = [
        pltpu.make_async_copy(order_hbm, order_ref, sem.at[0]),
        pltpu.make_async_copy(visc_hbm, visc_ref, sem.at[1]),
        pltpu.make_async_copy(mass_hbm, mass_ref, sem.at[2]),
        pltpu.make_async_copy(force_hbm.at[component], force_ref, sem.at[3]),
        pltpu.make_async_copy(cols_hbm.at[0], cols_ref, sem.at[4]),
    ]
    for copy in copies:
        copy.start()
    for copy in copies[:3]:
        copy.wait()
    cell_by_slot = (iota((elems, elems), 0) == order_ref[...]).astype(F32)
    perm = jnp.transpose(cell_by_slot).astype(BF16)
    coef = jnp.concatenate([visc_ref[...], mass_ref[...], jnp.zeros((6, elems), F32)], axis=0)
    high, mid, low = split3(coef)
    coef = dot_nn(high, perm) + dot_nn(mid, perm) + dot_nn(low, perm)
    pack_ref[nodes:, :] = coef
    for copy in copies[3:]:
        copy.wait()
    chunk = 128
    for at in range(0, nodes, chunk):
        piece = jnp.transpose(force_ref[:, at : at + chunk])
        high, mid, low = split3(piece)
        moved = dot_nn(high, perm) + dot_nn(mid, perm) + dot_nn(low, perm)
        moved = wide(cols_ref[at : at + chunk, :], elems) * moved
        pack_ref[at : at + chunk, :] = moved


def place_kernel(cap, order_ref, owner_ref, place_ref):
    elems = order_ref.shape[1]
    owners = elems // cap
    rows = max(8, owners)
    owner_row = owner_ref[...]
    match = (iota((rows, elems), 0) == owner_row).astype(F32)
    before = (iota((elems, elems), 0) < iota((elems, elems), 1)).astype(BF16)
    running = dot_nn(match.astype(BF16), before)
    rank = jnp.sum(match * running, axis=0, keepdims=True).astype(jnp.int32)
    dest = jnp.where(owner_row >= 0, owner_row * cap + rank, -1)
    to_dest = (iota((elems, elems), 0) == dest).astype(BF16)
    cell_by_slot = (iota((elems, elems), 0) == order_ref[...]).astype(BF16)
    place_ref[...] = dot_nt(to_dest, cell_by_slot).astype(BF16)


def lane_masks(rows):
    lane = iota((rows, TILE), 1)
    x_pos = lane % BX
    y_pos = lane // BX % BY
    return x_pos < BX - 1, x_pos > 0, y_pos < BY - 1, y_pos > 0, lane < LAYER


def pair(first, second, keep, back, stride, scale):
    up = pltpu.roll(first, TILE - stride, 1)
    down = pltpu.roll(second, stride, 1)
    if scale is None:
        return first + jnp.where(back, down, 0.0), second + jnp.where(keep, up, 0.0)
    return (
        jnp.where(back, scale * (first + down), first),
        jnp.where(keep, scale * (second + up), second),
    )


def share_xy(ref, tiles, scale=None):
    x_keep, x_back, y_keep, y_back, _ = lane_masks(FACE)
    y_keep, y_back = y_keep[:NP], y_back[:NP]
    for t in tiles:
        low = ref[t, pl.ds(0, FACE, stride=NP), :]
        high = ref[t, pl.ds(NP - 1, FACE, stride=NP), :]
        low, high = pair(low, high, x_keep, x_back, 1, scale)
        ref[t, pl.ds(0, FACE, stride=NP), :] = low
        ref[t, pl.ds(NP - 1, FACE, stride=NP), :] = high
        for k in range(NP):
            first = pl.ds(k * FACE, NP)
            last = pl.ds(k * FACE + FACE - NP, NP)
            low, high = pair(ref[t, first, :], ref[t, last, :], y_keep, y_back, BX, scale)
            ref[t, first, :] = low
            ref[t, last, :] = high


def load_block(ref, n, rows):
    return jnp.concatenate([ref[2 * n, rows, :], ref[2 * n + 1, rows, :]], axis=1)


def save_block(ref, n, rows, value):
    ref[2 * n, rows, :] = value[:, :TILE]
    ref[2 * n + 1, rows, :] = value[:, TILE:]


def share_z(ref, tiles):
    lower = lane_masks(FACE)[4]
    first = pl.ds(0, FACE)
    last = pl.ds((NP - 1) * FACE, FACE)
    lows = [ref[t, first, :] for t in tiles]
    highs = [ref[t, last, :] for t in tiles]
    low_roll = [pltpu.roll(v, LAYER, 1) for v in lows] + [jnp.zeros((FACE, TILE), F32)]
    high_roll = [jnp.zeros((FACE, TILE), F32)] + [pltpu.roll(v, LAYER, 1) for v in highs]
    for n, t in enumerate(tiles):
        up = jnp.where(lower, low_roll[n], low_roll[n + 1])
        down = jnp.where(lower, high_roll[n], high_roll[n + 1])
        ref[t, last, :] = highs[n] + up
        ref[t, first, :] = lows[n] + down


def stage_kernel(own_ref, cols_ref, raw_ref, rhs_ref, jac_ref):
    nodes = cols_ref.shape[1]
    elems = own_ref.shape[1]
    raw_ref[nodes:, :] = own_ref[nodes:, :]

    @pl.loop(0, NP)
    def _(k):
        rows = pl.ds(pl.multiple_of(k * FACE, FACE), FACE)
        value = own_ref[rows, :]
        raw_ref[rows, :] = value
        save_block(rhs_ref, 0, rows, value)
        w_col = wide(cols_ref[0, rows, :], elems)
        d_col = wide(cols_ref[1, rows, :], elems)
        visc = own_ref[nodes : nodes + 1, :]
        mass = own_ref[nodes + 1 : nodes + 2, :]
        save_block(jac_ref, 0, rows, visc * d_col + mass * w_col)

    share_xy(rhs_ref, [0, 1])
    share_xy(jac_ref, [0, 1])


def krylov_kernel(
    diff, bound, own_ref, rhs_ref, jac_ref, a_ref, b_ref, kmat_ref, cols_ref,
    basis_ref, near_ref, message_ref,
    work, coef, inv, vec, ghost, even, odd, prod, dots_ref,
):
    nodes = cols_ref.shape[1]
    elems = own_ref.shape[1]
    half = nodes // 2
    steps = ITERS
    odd_part = lax.axis_index("dom") % 2 > 0
    wide_tile = pl.ds(0, TILE)
    high_tile = pl.ds(TILE, TILE)

    def gather(rows, out_near, out_far):
        a_low, a_high = a_ref[rows, wide_tile], a_ref[rows, high_tile]
        b_low, b_high = b_ref[rows, wide_tile], b_ref[rows, high_tile]
        out_near(
            jnp.where(odd_part, a_high, b_high), jnp.where(odd_part, b_low, a_low)
        )
        out_far(
            jnp.where(odd_part, a_low, b_low), jnp.where(odd_part, b_high, a_high)
        )

    def store(ref, n, rows):
        def put(*parts):
            save_block(ref, n, rows, parts[0] if len(parts) == 1 else jnp.concatenate(parts, axis=1))
        return put

    def store_coef(n):
        def put(*parts):
            coef[n] = parts[0] if len(parts) == 1 else jnp.concatenate(parts, axis=1)
        return put

    tail = pl.ds(nodes, own_ref.shape[0] - nodes)
    coef[0] = own_ref[tail, :]
    gather(tail, store_coef(1), store_coef(2))

    @pl.loop(0, NP)
    def _(k):
        rows = pl.ds(pl.multiple_of(k * FACE, FACE), FACE)
        gather(rows, store(work, 1, rows), store(work, 2, rows))
        for t in range(2):
            work[t, rows, :] = rhs_ref[t, rows, :]
            inv[t, rows, :] = jac_ref[t, rows, :]
        w_col = wide(cols_ref[0, rows, :], elems)
        d_col = wide(cols_ref[1, rows, :], elems)
        for n in range(1, 3):
            save_block(inv, n, rows, coef[n, 0:1, :] * d_col + coef[n, 1:2, :] * w_col)

    far_tiles = [4, 2, 0, 1, 3, 5]
    near_tiles = far_tiles[1:5]
    share_xy(work, [2, 3, 4, 5])
    share_z(work, far_tiles)
    share_xy(inv, [2, 3, 4, 5])
    share_z(inv, far_tiles)

    @pl.loop(0, NP)
    def _(k):
        rows = pl.ds(pl.multiple_of(k * FACE, FACE), FACE)
        for n in range(3):
            total = load_block(inv, n, rows)
            recip = jnp.where(total > 0.0, 1.0 / total, 0.0)
            save_block(inv, n, rows, recip)
            value = recip * load_block(work, n, rows)
            if n == 0:
                basis_ref[0, rows, :] = value
            elif n == 1:
                ghost[0, rows, :] = value
            else:
                vec[rows, :] = value

    def vector(m, n, rows):
        if n == 0:
            return basis_ref[m, rows, :]
        return ghost[m, rows, :] if n == 1 else vec[rows, :]

    dots_ref[...] = jnp.zeros_like(dots_ref)

    def fold(value):
        rows, lanes = value.shape
        total = jnp.sum(value.reshape(rows // 8, 8, lanes), axis=0)
        return sum(total[:, at : at + TILE] for at in range(0, lanes, TILE))

    def apply(m, n):
        @pl.loop(0, NP // 2)
        def _(k):
            top = pl.ds(pl.multiple_of(k * FACE, FACE), FACE)
            bottom = pl.ds(pl.multiple_of((NP - 1 - k) * FACE, FACE), FACE)
            v_top = vector(m, n, top)
            v_bottom = vector(m, n, bottom)
            for part, ref in ((v_top + v_bottom, even), (v_top - v_bottom, odd)):
                high = part.astype(BF16)
                ref[0, top, :] = high
                ref[1, top, :] = (part - high.astype(F32)).astype(BF16)

        for parity, ref in ((0, even), (1, odd)):
            base = 3 * parity
            prod[parity] = (
                dot_nn(kmat_ref[base + 1], ref[1])
                + dot_nn(kmat_ref[base + 2], ref[0])
                + dot_nn(kmat_ref[base], ref[1])
                + dot_nn(kmat_ref[base + 1], ref[0])
                + dot_nn(kmat_ref[base], ref[0])
            )

        @pl.loop(0, NP // 2)
        def _(k):
            top = pl.ds(pl.multiple_of(k * FACE, FACE), FACE)
            bottom = pl.ds(pl.multiple_of((NP - 1 - k) * FACE, FACE), FACE)
            p_even = prod[0, top, :]
            p_odd = prod[1, top, :]
            w_top = wide(cols_ref[0, top, :], elems)
            w_bottom = wide(cols_ref[0, bottom, :], elems)
            visc = coef[n, 0:1, :]
            mass = coef[n, 1:2, :]
            q_top = visc * (p_even + p_odd) + mass * (w_top * vector(m, n, top))
            q_bottom = visc * (p_even - p_odd) + mass * (w_bottom * vector(m, n, bottom))
            if m + 1 < steps:
                save_block(work, n, top, q_top)
                save_block(work, n, bottom, q_bottom)
            if n == 0:
                for i in range(m + 1):
                    dots_ref[m * (m + 1) // 2 + i] += fold(
                        basis_ref[i, top, :] * q_top + basis_ref[i, bottom, :] * q_bottom
                    )
                at = steps * (steps + 1) // 2 + m
                dots_ref[at] += fold(
                    basis_ref[m, top, :] * own_ref[top, :]
                    + basis_ref[m, bottom, :] * own_ref[bottom, :]
                )

    for m in range(steps):
        if m + 1 == steps:
            apply(m, 0)
            continue
        blocks = (0, 1, 2) if m == 0 else (0, 1)
        for n in blocks:
            apply(m, n)
        tiles = far_tiles if m == 0 else near_tiles
        share_xy(work, tiles)
        share_z(work, tiles)
        outs = (0, 1) if m + 2 < steps else (0,)

        @pl.loop(0, NP)
        def _(k):
            rows = pl.ds(pl.multiple_of(k * FACE, FACE), FACE)
            for n in outs:
                value = (2.0 / bound) * (load_block(inv, n, rows) * load_block(work, n, rows)) - vector(m, n, rows)
                if m > 0:
                    value = value + value - vector(m - 1, n, rows)
                if n == 0:
                    basis_ref[m + 1, rows, :] = value
                else:
                    ghost[m + 1, rows, :] = value

    def plane(load, row):
        total = None
        for k in range(NP):
            term = float(diff[row, k]) * load(k)
            total = term if total is None else total + term
        return total

    lower = lane_masks(FACE)[4]

    def rows_of(k):
        return pl.ds(k * FACE, FACE)

    last = steps - 1
    bottom = plane(lambda k: basis_ref[last, rows_of(k), wide_tile], 0)
    top = plane(lambda k: basis_ref[last, rows_of(k), high_tile], NP - 1)
    message_ref[:FACE] = jnp.where(lower, bottom, top)
    message_ref[FACE:] = jnp.sum(dots_ref[...], axis=1)
    for m in range(steps - 1):
        below = plane(lambda k: ghost[m, rows_of(k), wide_tile], NP - 1)
        above = plane(lambda k: ghost[m, rows_of(k), high_tile], 0)
        near_ref[m] = jnp.where(lower, above, below)


def solve_coefficients(sums):
    size = ITERS
    gram = {}
    for j in range(size):
        for i in range(j + 1):
            at = j * (j + 1) // 2 + i
            gram[j, i] = sums[at : at + 1]
    at = size * (size + 1) // 2
    right = [sums[at + i : at + i + 1] for i in range(size)]
    lower, recip = {}, []
    reduced = {}
    for k in range(size):
        for i in range(k, size):
            value = gram[i, k]
            for m in range(k):
                value = value - lower[i, m] * reduced[k, m]
            reduced[i, k] = value
        pivot = reduced[k, k]
        usable = pivot > 1e-7 * gram[k, k]
        inverse = jnp.where(usable, 1.0 / jnp.where(usable, pivot, 1.0), 0.0)
        recip.append(inverse)
        for i in range(k + 1, size):
            lower[i, k] = reduced[i, k] * inverse
    for k in range(size):
        for m in range(k):
            right[k] = right[k] - lower[k, m] * right[m]
    out = [None] * size
    for k in reversed(range(size)):
        value = right[k] * recip[k]
        for m in range(k + 1, size):
            value = value - lower[m, k] * out[m]
        out[k] = value
    return out


def gradient_kernel(
    diff, sum_a_ref, sum_b_ref, basis_ref, near_ref, fa_ref, fb_ref, dcol_ref,
    *rest,
):
    *grad_refs, vel_ref, work = rest
    elems = basis_ref.shape[2]
    quarter = grad_refs[0].shape[1]
    group = lax.axis_index("grp")
    scalars = jnp.sum(sum_a_ref[...] + sum_b_ref[...], axis=1, keepdims=True)
    part = lax.axis_index("dom")
    parts = lax.axis_size("dom")
    weights = solve_coefficients(scalars)
    tiles = range(elems // TILE)

    @pl.loop(0, NP)
    def _(k):
        rows = pl.ds(pl.multiple_of(k * FACE, FACE), FACE)
        total = weights[0] * basis_ref[0, rows, :]
        for m in range(1, ITERS):
            total = total + weights[m] * basis_ref[m, rows, :]
        vel_ref[rows, :] = total

    lower = lane_masks(FACE)[4]
    x_keep, x_back, y_keep, y_back, _ = lane_masks(FACE)
    odd_part = lax.axis_index("dom") % 2 > 0
    from_above = jnp.where(odd_part, fb_ref[:FACE], fa_ref[:FACE])
    from_below = jnp.where(odd_part, fa_ref[:FACE], fb_ref[:FACE])
    near = weights[ITERS - 1] * jnp.where(lower, from_above, from_below)
    for m in range(ITERS - 1):
        near = near + weights[m] * near_ref[m]
    near = pltpu.roll(near, LAYER, 1)

    def finish(direction, scale):
        share_xy(work, tiles, 0.5)
        if direction == 2:
            first = pl.ds(0, FACE)
            last = pl.ds((NP - 1) * FACE, FACE)
            lows = [work[t, first, :] for t in tiles]
            highs = [work[t, last, :] for t in tiles]
            low_roll = [pltpu.roll(v, LAYER, 1) for v in lows] + [near]
            high_roll = [near] + [pltpu.roll(v, LAYER, 1) for v in highs]
            count = len(tiles)
            for n in tiles:
                up = jnp.where(lower, low_roll[n], low_roll[n + 1])
                down = jnp.where(lower, high_roll[n], high_roll[n + 1])
                high_mean = 0.5 * (highs[n] + up)
                low_mean = 0.5 * (lows[n] + down)
                if n == count - 1:
                    edge = jnp.logical_and(jnp.logical_not(lower), part == parts - 1)
                    high_mean = jnp.where(edge, highs[n], high_mean)
                if n == 0:
                    edge = jnp.logical_and(lower, part == 0)
                    low_mean = jnp.where(edge, lows[n], low_mean)
                work[n, last, :] = high_mean
                work[n, first, :] = low_mean
        for turn, grad_ref in enumerate(grad_refs):
            start = pl.multiple_of(jnp.bitwise_xor(group, turn) * quarter, quarter)
            value = load_block(work, 0, pl.ds(start, quarter)) * scale
            grad_ref[direction] = value.astype(BF16)

    @pl.loop(0, NP)
    def _(k):
        rows = pl.ds(pl.multiple_of(k * FACE, FACE), FACE)
        value = vel_ref[rows, :].reshape(NP, NP, elems)
        total = wide(dcol_ref[0], elems)[None] * value
        for shift in range(1, NP):
            total = total + wide(dcol_ref[shift], elems)[None] * pltpu.roll(value, NP - shift, 1)
        save_block(work, 0, rows, total.reshape(FACE, elems))

    finish(0, 1.0 / NP)

    @pl.loop(0, NP)
    def _(k):
        rows = pl.ds(pl.multiple_of(k * FACE, FACE), FACE)
        value = vel_ref[rows, :].reshape(NP, NP, elems)
        for j in range(NP):
            total = float(diff[j, 0]) * value[0]
            for m in range(1, NP):
                total = total + float(diff[j, m]) * value[m]
            save_block(work, 0, pl.ds(pl.multiple_of(k * FACE + j * NP, NP), NP), total)

    finish(1, 1.0 / NP)

    @pl.loop(0, NP)
    def _(j):
        planes = [vel_ref[pl.ds(pl.multiple_of(m * FACE + j * NP, NP), NP), :] for m in range(NP)]
        for k in range(NP):
            total = float(diff[k, 0]) * planes[0]
            for m in range(1, NP):
                total = total + float(diff[k, m]) * planes[m]
            save_block(work, 0, pl.ds(pl.multiple_of(k * FACE + j * NP, NP), NP), total)

    finish(2, 1.0 / NP)


def slots_kernel(order_ref, vel_ref, out_ref):
    elems = order_ref.shape[1]
    cell_by_slot = (iota((elems, elems), 0) == order_ref[...]).astype(F32)
    pick = jnp.transpose(cell_by_slot).astype(BF16)
    high, mid, low = split3(vel_ref[...])
    out_ref[...] = dot_nt(pick, high) + dot_nt(pick, mid) + dot_nt(pick, low)


def middle_eigenvalue(jac):
    strain = [[0.5 * (jac[a][b] + jac[b][a]) for b in range(3)] for a in range(3)]
    spin = [[0.5 * (jac[a][b] - jac[b][a]) for b in range(3)] for a in range(3)]
    mat = [[None] * 3 for _ in range(3)]
    for a in range(3):
        for b in range(a, 3):
            total = strain[a][0] * strain[0][b] + spin[a][0] * spin[0][b]
            for c in (1, 2):
                total = total + strain[a][c] * strain[c][b] + spin[a][c] * spin[c][b]
            mat[a][b] = total
            mat[b][a] = total
    peak = jnp.maximum(jnp.abs(mat[0][1]), jnp.maximum(jnp.abs(mat[0][2]), jnp.abs(mat[1][2])))
    for a in range(3):
        peak = jnp.maximum(peak, jnp.abs(mat[a][a]))
    peak = jnp.where(peak > 0.0, peak, 1.0)
    shrink = 1.0 / peak
    for a in range(3):
        for b in range(a, 3):
            mat[a][b] = mat[b][a] = mat[a][b] * shrink
    for _ in range(SWEEPS):
        for p, q, r in ((0, 1, 2), (0, 2, 1), (1, 2, 0)):
            pivot = mat[p][q]
            first, second = mat[p][p], mat[q][q]
            gap = 0.5 * (first - second)
            norm = pivot * pivot + gap * gap
            inv_norm = lax.rsqrt(jnp.maximum(norm, 1e-37))
            middle = 0.5 * (first + second)
            radius = norm * inv_norm
            turned = norm > 0.0
            cos_two = jnp.where(turned, gap * inv_norm, 1.0)
            half_sin = (0.5 * pivot) * inv_norm
            lead = 0.5 + 0.5 * jnp.abs(cos_two)
            inv_big = lax.rsqrt(lead)
            big = lead * inv_big
            small = half_sin * inv_big
            forward = cos_two >= 0.0
            cosine = jnp.where(forward, big, jnp.abs(small))
            sine = jnp.where(forward, small, jnp.where(pivot < 0.0, -big, big))
            mat[p][p] = middle + radius
            mat[q][q] = middle - radius
            mat[p][q] = mat[q][p] = None
            side_p, side_q = mat[r][p], mat[r][q]
            if side_p is None:
                new_p, new_q = sine * side_q, cosine * side_q
            elif side_q is None:
                new_p, new_q = cosine * side_p, -(sine * side_p)
            else:
                new_p = cosine * side_p + sine * side_q
                new_q = cosine * side_q - sine * side_p
            mat[r][p] = mat[p][r] = new_p
            mat[r][q] = mat[q][r] = new_q
    d0, d1, d2 = mat[0][0], mat[1][1], mat[2][2]
    largest = jnp.maximum(jnp.maximum(d0, d1), d2)
    smallest = jnp.minimum(jnp.minimum(d0, d1), d2)
    return (d0 + d1 + d2 - largest - smallest) * peak


def vortex_kernel(*refs):
    *grad_refs, place_ref, out_ref, value = refs
    rows_all = grad_refs[0].shape[1]
    group = lax.axis_index("grp")

    def component(c, d, rows):
        turn = jnp.bitwise_xor(group, c)
        out = grad_refs[-1][d, rows, :].astype(F32)
        for n in reversed(range(len(grad_refs) - 1)):
            out = jnp.where(turn == n, grad_refs[n][d, rows, :].astype(F32), out)
        return out

    step = 16

    @pl.loop(0, rows_all // step)
    def _(n):
        rows = pl.ds(pl.multiple_of(n * step, step), step)
        jac = [[component(c, d, rows) for d in range(3)] for c in range(3)]
        value[rows, :] = middle_eigenvalue(jac)

    high, mid, low = split3(value[...])
    place = place_ref[...]
    moved = dot_nt(place, high) + dot_nt(place, mid) + dot_nt(place, low)
    owners, cap = out_ref.shape[0], out_ref.shape[1]
    used = place.shape[0] // cap
    out_ref[: owners - used] = jnp.zeros((owners - used,) + out_ref.shape[1:], F32)
    out_ref[owners - used :] = moved.reshape((used,) + out_ref.shape[1:])


def final_kernel(vortex_ref, vel_ref, out_ref):
    quarters = vortex_ref.shape[0]
    quarter = vortex_ref.shape[2]

    last = lax.axis_index("grp") == lax.axis_size("grp") - 1

    @pl.when(last)
    def _():
        for q in range(quarters):
            out_ref[0, :, q * quarter : (q + 1) * quarter] = vortex_ref[q]

    @pl.when(jnp.logical_not(last))
    def _():
        out_ref[0] = vel_ref[...]


PREP_LIMIT = 67043328 - 2600 * 1024
GRANT = pltpu.CompilerParams(vmem_limit_bytes=24 * 2**20)


def vmem():
    return pl.BlockSpec(memory_space=pltpu.VMEM)


def cost(flops, size):
    return pl.CostEstimate(flops=flops, bytes_accessed=size, transcendentals=0)


def per_device(forcing, viscosity, mass_coef, element_order, owner):
    elems = viscosity.shape[0]
    nodes = forcing.shape[2]
    parts = lax.axis_size("dom")
    groups = lax.axis_size("grp")
    cap = elems // parts
    quarter = nodes // groups
    diff, kmat_np, cols_np, dcol_np, bound = host_tables()
    kmat = jnp.asarray(kmat_np, BF16)
    cols = jnp.asarray(cols_np)
    dcol = jnp.asarray(dcol_np)
    sds = jax.ShapeDtypeStruct

    pack = pl.pallas_call(
        prep_kernel,
        in_specs=[pl.BlockSpec(memory_space=pltpu.HBM)] * 5,
        out_specs=vmem(),
        out_shape=sds((nodes + 8, elems), F32),
        scratch_shapes=[
            pltpu.VMEM((elems, nodes), F32),
            pltpu.VMEM((1, elems), jnp.int32),
            pltpu.VMEM((1, elems), F32),
            pltpu.VMEM((1, elems), F32),
            pltpu.VMEM((nodes, TILE), F32),
            pltpu.SemaphoreType.DMA((5,)),
        ],
        cost_estimate=cost(10**9, 2 * 10**6),
        compiler_params=pltpu.CompilerParams(vmem_limit_bytes=PREP_LIMIT),
        name="prep",
    )(forcing, element_order, viscosity[None], mass_coef[None], cols)

    swap_a = [(i, i ^ 1) for i in range(parts) if i ^ 1 < parts]
    swap_b = [(i, ((i - 1) ^ 1) + 1) for i in range(1, parts - 1)]
    ghost_b = lax.ppermute(pack, "dom", swap_b)
    ghost_a = lax.ppermute(pack, "dom", swap_a)

    raw, rhs_xy, jac_xy = pl.pallas_call(
        stage_kernel,
        in_specs=[vmem()] * 2,
        out_specs=[vmem()] * 3,
        out_shape=[
            sds((nodes + 8, elems), F32),
            sds((2, nodes, TILE), F32),
            sds((2, nodes, TILE), F32),
        ],
        cost_estimate=cost(10**9, 2 * 10**6),
        compiler_params=GRANT,
        name="stage",
    )(pack, cols)

    place = pl.pallas_call(
        lambda *refs: place_kernel(cap, *refs),
        in_specs=[vmem(), vmem()],
        out_specs=vmem(),
        out_shape=sds((elems, elems), BF16),
        cost_estimate=cost(10**9, 2 * 10**6),
        compiler_params=GRANT,
        name="place",
    )(element_order, owner)

    basis, near, message = pl.pallas_call(
        lambda *refs: krylov_kernel(diff, bound, *refs),
        in_specs=[vmem()] * 7,
        out_specs=[vmem()] * 3,
        out_shape=[
            sds((ITERS, nodes, elems), F32),
            sds((ITERS - 1, FACE, TILE), F32),
            sds((FACE + 16, TILE), F32),
        ],
        scratch_shapes=[
            pltpu.VMEM((6, nodes, TILE), F32),
            pltpu.VMEM((3, 8, elems), F32),
            pltpu.VMEM((6, nodes, TILE), F32),
            pltpu.VMEM((nodes, elems), F32),
            pltpu.VMEM((ITERS - 1, nodes, elems), F32),
            pltpu.VMEM((2, nodes // 2, elems), BF16),
            pltpu.VMEM((2, nodes // 2, elems), BF16),
            pltpu.VMEM((2, nodes // 2, elems), F32),
            pltpu.VMEM((16, 8, TILE), F32),
        ],
        cost_estimate=cost(10**10, 10**7),
        compiler_params=GRANT,
        name="krylov",
    )(raw, rhs_xy, jac_xy, ghost_a, ghost_b, kmat, cols)

    face_a = lax.ppermute(message, "dom", swap_a)
    face_b = lax.ppermute(message, "dom", swap_b)
    pending = (message[FACE:], face_a[FACE:])
    reach = 2
    while reach < parts:
        sums = pending[0] + pending[1]
        pending = (sums, lax.ppermute(sums, "dom", [(i, i ^ reach) for i in range(parts)]))
        reach *= 2

    *grads, vel = pl.pallas_call(
        lambda *refs: gradient_kernel(diff, *refs),
        in_specs=[vmem()] * 7,
        out_specs=[vmem()] * (groups + 1),
        out_shape=[sds((3, quarter, elems), BF16)] * groups + [sds((nodes, elems), F32)],
        scratch_shapes=[pltpu.VMEM((2, nodes, TILE), F32)],
        cost_estimate=cost(10**9, 4 * 10**6),
        compiler_params=GRANT,
        name="gradient",
    )(*pending, basis, near, face_a, face_b, dcol)

    exchanged = [grads[0]] + [
        lax.ppermute(grads[turn], "grp", [(i, i ^ turn) for i in range(groups)])
        for turn in range(1, groups)
    ]

    vel_slot = pl.pallas_call(
        slots_kernel,
        in_specs=[vmem(), vmem()],
        out_specs=vmem(),
        out_shape=sds((elems, nodes), F32),
        cost_estimate=cost(10**9, 2 * 10**6),
        compiler_params=GRANT,
        name="slots",
    )(element_order, vel)

    packed = pl.pallas_call(
        vortex_kernel,
        in_specs=[vmem()] * (groups + 1),
        out_specs=vmem(),
        out_shape=sds((groups * parts, cap, quarter), F32),
        scratch_shapes=[pltpu.VMEM((quarter, elems), F32)],
        cost_estimate=cost(10**9, 2 * 10**6),
        compiler_params=GRANT,
        name="vortex",
    )(*exchanged, place)

    received = lax.all_to_all(
        packed, ("grp", "dom"), split_axis=0, concat_axis=0, tiled=True
    )
    return pl.pallas_call(
        final_kernel,
        in_specs=[vmem(), vmem()],
        out_specs=vmem(),
        out_shape=sds((1, elems, nodes), F32),
        cost_estimate=cost(10**6, 2 * 10**6),
        compiler_params=GRANT,
        name="final",
    )(received.reshape(groups, elems, quarter), vel_slot)


def solution(mesh):
    in_specs = (P(None, "dom", None), P("dom"), P("dom"), P("dom", None), P("dom", None))
    out_specs = P("grp", "dom", None)
    return jax.shard_map(
        per_device, mesh=mesh, in_specs=in_specs, out_specs=out_specs, check_vma=False
    )
```

```python
import jax
import jax.numpy as jnp
import numpy as np
from jax import lax
from jax.experimental import pallas as pl
from jax.experimental.pallas import tpu as pltpu
from jax.sharding import PartitionSpec as P

NP = 8
BX = 8
BY = 8
ITERS = 4
SWEEPS = 4
FACE = NP * NP
LAYER = BX * BY
TILE = 2 * LAYER
F32 = jnp.float32
BF16 = jnp.bfloat16


def legendre_values(points, node_count):
    legendre = np.zeros((points.shape[0], node_count))
    legendre[:, 0] = 1.0
    legendre[:, 1] = points
    for poly_order in range(2, node_count):
        legendre[:, poly_order] = (
            (2 * poly_order - 1) * points * legendre[:, poly_order - 1]
            - (poly_order - 1) * legendre[:, poly_order - 2]
        ) / poly_order
    return legendre


def lobatto_table(node_count):
    degree = node_count - 1
    points = np.cos(np.pi * np.arange(node_count) / degree)
    for attempt in range(60):
        legendre = legendre_values(points, node_count)
        points = points - (points * legendre[:, degree] - legendre[:, degree - 1]) / (
            node_count * legendre[:, degree]
        )
    points = points[::-1].copy()
    end_values = legendre_values(points, node_count)[:, degree]
    weights = 2.0 / (degree * node_count * end_values * end_values)
    spacing = points[:, None] - points[None, :] + np.eye(node_count)
    diff_matrix = end_values[:, None] / end_values[None, :] / spacing
    diff_matrix = diff_matrix * (1.0 - np.eye(node_count))
    diff_matrix[0, 0] = -degree * node_count / 4.0
    diff_matrix[-1, -1] = degree * node_count / 4.0
    return (weights, diff_matrix)


def operator_tables(node_count):
    weights, diff_matrix = lobatto_table(node_count)
    identity = np.eye(node_count)
    weight_cube = (
        weights[:, None, None] * weights[None, :, None] * weights[None, None, :]
    ).reshape(-1)
    directional = [
        np.kron(identity, np.kron(identity, diff_matrix)),
        np.kron(identity, np.kron(diff_matrix, identity)),
        np.kron(diff_matrix, np.kron(identity, identity)),
    ]
    stiffness = np.zeros((node_count**3, node_count**3))
    for direction_matrix in directional:
        stiffness = stiffness + direction_matrix.T @ (weight_cube[:, None] * direction_matrix)
    return diff_matrix, weight_cube, stiffness


def split3_np(table):
    parts = []
    rest = np.asarray(table, np.float64)
    for _ in range(3):
        part = rest.astype(np.float32).astype(BF16)
        parts.append(part)
        rest = rest - part.astype(np.float64)
    return parts


def host_tables():
    diff_matrix, weight_cube, stiffness = operator_tables(NP)
    half = FACE * NP // 2
    flip = np.concatenate([np.arange(FACE) + FACE * k for k in range(NP - 1, NP // 2 - 1, -1)])
    top = stiffness[:half, :half]
    cross = stiffness[:half][:, flip]
    even = split3_np(0.5 * (top + cross))
    odd = split3_np(0.5 * (top - cross))
    kmat = np.stack(even + odd)
    diag = np.diag(stiffness)
    scaled = stiffness / np.sqrt(diag[:, None] * diag[None, :])
    bound = max(1.0, float(np.linalg.eigvalsh(scaled)[-1]))
    cols = np.stack([weight_cube, diag]).astype(np.float32)
    cols = np.ascontiguousarray(np.broadcast_to(cols[:, :, None], cols.shape + (TILE,)))
    dcol = np.zeros((NP, NP, TILE), np.float32)
    for shift in range(NP):
        for row in range(NP):
            dcol[shift, row] = diff_matrix[row, (row + shift) % NP]
    return diff_matrix, kmat, cols, dcol, bound


def split3(value):
    high = value.astype(BF16)
    rest = value - high.astype(F32)
    mid = rest.astype(BF16)
    low = (rest - mid.astype(F32)).astype(BF16)
    return high, mid, low


def dot_nn(a, b):
    return jnp.dot(a, b, preferred_element_type=F32)


def dot_nt(a, b):
    return lax.dot_general(a, b, (((1,), (1,)), ((), ())), preferred_element_type=F32)


def iota(shape, dim):
    return lax.broadcasted_iota(jnp.int32, shape, dim)


def wide(col, lanes):
    return jnp.concatenate([col] * (lanes // col.shape[1]), axis=1)


def prep_kernel(
    force_hbm, order_hbm, visc_hbm, mass_hbm, cols_hbm, pack_ref,
    force_ref, order_ref, visc_ref, mass_ref, cols_ref, sem,
):
    elems = order_ref.shape[1]
    nodes = force_ref.shape[1]
    component = jnp.minimum(lax.axis_index("grp"), 2)
    copies = [
        pltpu.make_async_copy(order_hbm, order_ref, sem.at[0]),
        pltpu.make_async_copy(visc_hbm, visc_ref, sem.at[1]),
        pltpu.make_async_copy(mass_hbm, mass_ref, sem.at[2]),
        pltpu.make_async_copy(force_hbm.at[component], force_ref, sem.at[3]),
        pltpu.make_async_copy(cols_hbm.at[0], cols_ref, sem.at[4]),
    ]
    for copy in copies:
        copy.start()
    for copy in copies[:3]:
        copy.wait()
    cell_by_slot = (iota((elems, elems), 0) == order_ref[...]).astype(F32)
    perm = jnp.transpose(cell_by_slot).astype(BF16)
    coef = jnp.concatenate([visc_ref[...], mass_ref[...], jnp.zeros((6, elems), F32)], axis=0)
    high, mid, low = split3(coef)
    coef = dot_nn(high, perm) + dot_nn(mid, perm) + dot_nn(low, perm)
    pack_ref[nodes:, :] = coef
    for copy in copies[3:]:
        copy.wait()
    chunk = 128
    for at in range(0, nodes, chunk):
        piece = jnp.transpose(force_ref[:, at : at + chunk])
        high, mid, low = split3(piece)
        moved = dot_nn(high, perm) + dot_nn(mid, perm) + dot_nn(low, perm)
        moved = wide(cols_ref[at : at + chunk, :], elems) * moved
        pack_ref[at : at + chunk, :] = moved


def place_kernel(cap, order_ref, owner_ref, place_ref):
    elems = order_ref.shape[1]
    owners = elems // cap
    rows = max(8, owners)
    owner_row = owner_ref[...]
    match = (iota((rows, elems), 0) == owner_row).astype(F32)
    before = (iota((elems, elems), 0) < iota((elems, elems), 1)).astype(BF16)
    running = dot_nn(match.astype(BF16), before)
    rank = jnp.sum(match * running, axis=0, keepdims=True).astype(jnp.int32)
    dest = jnp.where(owner_row >= 0, owner_row * cap + rank, -1)
    to_dest = (iota((elems, elems), 0) == dest).astype(BF16)
    cell_by_slot = (iota((elems, elems), 0) == order_ref[...]).astype(BF16)
    place_ref[...] = dot_nt(to_dest, cell_by_slot).astype(BF16)


def lane_masks(rows):
    lane = iota((rows, TILE), 1)
    x_pos = lane % BX
    y_pos = lane // BX % BY
    return x_pos < BX - 1, x_pos > 0, y_pos < BY - 1, y_pos > 0, lane < LAYER


def pair(first, second, keep, back, stride, scale):
    up = pltpu.roll(first, TILE - stride, 1)
    down = pltpu.roll(second, stride, 1)
    if scale is None:
        return first + jnp.where(back, down, 0.0), second + jnp.where(keep, up, 0.0)
    return (
        jnp.where(back, scale * (first + down), first),
        jnp.where(keep, scale * (second + up), second),
    )


def share_xy(ref, tiles, scale=None):
    x_keep, x_back, y_keep, y_back, _ = lane_masks(FACE)
    y_keep, y_back = y_keep[:NP], y_back[:NP]
    for t in tiles:
        low = ref[t, pl.ds(0, FACE, stride=NP), :]
        high = ref[t, pl.ds(NP - 1, FACE, stride=NP), :]
        low, high = pair(low, high, x_keep, x_back, 1, scale)
        ref[t, pl.ds(0, FACE, stride=NP), :] = low
        ref[t, pl.ds(NP - 1, FACE, stride=NP), :] = high
        for k in range(NP):
            first = pl.ds(k * FACE, NP)
            last = pl.ds(k * FACE + FACE - NP, NP)
            low, high = pair(ref[t, first, :], ref[t, last, :], y_keep, y_back, BX, scale)
            ref[t, first, :] = low
            ref[t, last, :] = high


def load_block(ref, n, rows):
    return jnp.concatenate([ref[2 * n, rows, :], ref[2 * n + 1, rows, :]], axis=1)


def save_block(ref, n, rows, value):
    ref[2 * n, rows, :] = value[:, :TILE]
    ref[2 * n + 1, rows, :] = value[:, TILE:]


def share_z(ref, tiles):
    lower = lane_masks(FACE)[4]
    first = pl.ds(0, FACE)
    last = pl.ds((NP - 1) * FACE, FACE)
    lows = [ref[t, first, :] for t in tiles]
    highs = [ref[t, last, :] for t in tiles]
    low_roll = [pltpu.roll(v, LAYER, 1) for v in lows] + [jnp.zeros((FACE, TILE), F32)]
    high_roll = [jnp.zeros((FACE, TILE), F32)] + [pltpu.roll(v, LAYER, 1) for v in highs]
    for n, t in enumerate(tiles):
        up = jnp.where(lower, low_roll[n], low_roll[n + 1])
        down = jnp.where(lower, high_roll[n], high_roll[n + 1])
        ref[t, last, :] = highs[n] + up
        ref[t, first, :] = lows[n] + down


def stage_kernel(own_ref, cols_ref, raw_ref, rhs_ref, jac_ref):
    nodes = cols_ref.shape[1]
    elems = own_ref.shape[1]
    raw_ref[nodes:, :] = own_ref[nodes:, :]

    @pl.loop(0, NP)
    def _(k):
        rows = pl.ds(pl.multiple_of(k * FACE, FACE), FACE)
        value = own_ref[rows, :]
        raw_ref[rows, :] = value
        save_block(rhs_ref, 0, rows, value)
        w_col = wide(cols_ref[0, rows, :], elems)
        d_col = wide(cols_ref[1, rows, :], elems)
        visc = own_ref[nodes : nodes + 1, :]
        mass = own_ref[nodes + 1 : nodes + 2, :]
        save_block(jac_ref, 0, rows, visc * d_col + mass * w_col)

    share_xy(rhs_ref, [0, 1])
    share_xy(jac_ref, [0, 1])


def krylov_kernel(
    diff, bound, own_ref, rhs_ref, jac_ref, a_ref, b_ref, kmat_ref, cols_ref,
    basis_ref, near_ref, message_ref,
    work, coef, inv, vec, ghost, even, odd, prod, dots_ref,
):
    nodes = cols_ref.shape[1]
    elems = own_ref.shape[1]
    half = nodes // 2
    steps = ITERS
    odd_part = lax.axis_index("dom") % 2 > 0
    wide_tile = pl.ds(0, TILE)
    high_tile = pl.ds(TILE, TILE)

    def gather(rows, out_near, out_far):
        a_low, a_high = a_ref[rows, wide_tile], a_ref[rows, high_tile]
        b_low, b_high = b_ref[rows, wide_tile], b_ref[rows, high_tile]
        out_near(
            jnp.where(odd_part, a_high, b_high), jnp.where(odd_part, b_low, a_low)
        )
        out_far(
            jnp.where(odd_part, a_low, b_low), jnp.where(odd_part, b_high, a_high)
        )

    def store(ref, n, rows):
        def put(*parts):
            save_block(ref, n, rows, parts[0] if len(parts) == 1 else jnp.concatenate(parts, axis=1))
        return put

    def store_coef(n):
        def put(*parts):
            coef[n] = parts[0] if len(parts) == 1 else jnp.concatenate(parts, axis=1)
        return put

    tail = pl.ds(nodes, own_ref.shape[0] - nodes)
    coef[0] = own_ref[tail, :]
    gather(tail, store_coef(1), store_coef(2))

    @pl.loop(0, NP)
    def _(k):
        rows = pl.ds(pl.multiple_of(k * FACE, FACE), FACE)
        gather(rows, store(work, 1, rows), store(work, 2, rows))
        for t in range(2):
            work[t, rows, :] = rhs_ref[t, rows, :]
            inv[t, rows, :] = jac_ref[t, rows, :]
        w_col = wide(cols_ref[0, rows, :], elems)
        d_col = wide(cols_ref[1, rows, :], elems)
        for n in range(1, 3):
            save_block(inv, n, rows, coef[n, 0:1, :] * d_col + coef[n, 1:2, :] * w_col)

    far_tiles = [4, 2, 0, 1, 3, 5]
    near_tiles = far_tiles[1:5]
    share_xy(work, [2, 3, 4, 5])
    share_z(work, far_tiles)
    share_xy(inv, [2, 3, 4, 5])
    share_z(inv, far_tiles)

    @pl.loop(0, NP)
    def _(k):
        rows = pl.ds(pl.multiple_of(k * FACE, FACE), FACE)
        for n in range(3):
            total = load_block(inv, n, rows)
            recip = jnp.where(total > 0.0, 1.0 / total, 0.0)
            save_block(inv, n, rows, recip)
            value = recip * load_block(work, n, rows)
            if n == 0:
                basis_ref[0, rows, :] = value
            elif n == 1:
                ghost[0, rows, :] = value
            else:
                vec[rows, :] = value

    def vector(m, n, rows):
        if n == 0:
            return basis_ref[m, rows, :]
        return ghost[m, rows, :] if n == 1 else vec[rows, :]

    dots_ref[...] = jnp.zeros_like(dots_ref)

    def fold(value):
        rows, lanes = value.shape
        total = jnp.sum(value.reshape(rows // 8, 8, lanes), axis=0)
        return sum(total[:, at : at + TILE] for at in range(0, lanes, TILE))

    def apply(m, n):
        @pl.loop(0, NP // 2)
        def _(k):
            top = pl.ds(pl.multiple_of(k * FACE, FACE), FACE)
            bottom = pl.ds(pl.multiple_of((NP - 1 - k) * FACE, FACE), FACE)
            v_top = vector(m, n, top)
            v_bottom = vector(m, n, bottom)
            for part, ref in ((v_top + v_bottom, even), (v_top - v_bottom, odd)):
                high = part.astype(BF16)
                ref[0, top, :] = high
                ref[1, top, :] = (part - high.astype(F32)).astype(BF16)

        for parity, ref in ((0, even), (1, odd)):
            base = 3 * parity
            prod[parity] = (
                dot_nn(kmat_ref[base + 1], ref[1])
                + dot_nn(kmat_ref[base + 2], ref[0])
                + dot_nn(kmat_ref[base], ref[1])
                + dot_nn(kmat_ref[base + 1], ref[0])
                + dot_nn(kmat_ref[base], ref[0])
            )

        @pl.loop(0, NP // 2)
        def _(k):
            top = pl.ds(pl.multiple_of(k * FACE, FACE), FACE)
            bottom = pl.ds(pl.multiple_of((NP - 1 - k) * FACE, FACE), FACE)
            p_even = prod[0, top, :]
            p_odd = prod[1, top, :]
            w_top = wide(cols_ref[0, top, :], elems)
            w_bottom = wide(cols_ref[0, bottom, :], elems)
            visc = coef[n, 0:1, :]
            mass = coef[n, 1:2, :]
            q_top = visc * (p_even + p_odd) + mass * (w_top * vector(m, n, top))
            q_bottom = visc * (p_even - p_odd) + mass * (w_bottom * vector(m, n, bottom))
            if m + 1 < steps:
                save_block(work, n, top, q_top)
                save_block(work, n, bottom, q_bottom)
            if n == 0:
                for i in range(m + 1):
                    dots_ref[m * (m + 1) // 2 + i] += fold(
                        basis_ref[i, top, :] * q_top + basis_ref[i, bottom, :] * q_bottom
                    )
                at = steps * (steps + 1) // 2 + m
                dots_ref[at] += fold(
                    basis_ref[m, top, :] * own_ref[top, :]
                    + basis_ref[m, bottom, :] * own_ref[bottom, :]
                )

    for m in range(steps):
        if m + 1 == steps:
            apply(m, 0)
            continue
        blocks = (0, 1, 2) if m == 0 else (0, 1)
        for n in blocks:
            apply(m, n)
        tiles = far_tiles if m == 0 else near_tiles
        share_xy(work, tiles)
        share_z(work, tiles)
        outs = (0, 1) if m + 2 < steps else (0,)

        @pl.loop(0, NP)
        def _(k):
            rows = pl.ds(pl.multiple_of(k * FACE, FACE), FACE)
            for n in outs:
                value = (2.0 / bound) * (load_block(inv, n, rows) * load_block(work, n, rows)) - vector(m, n, rows)
                if m > 0:
                    value = value + value - vector(m - 1, n, rows)
                if n == 0:
                    basis_ref[m + 1, rows, :] = value
                else:
                    ghost[m + 1, rows, :] = value

    def plane(load, row):
        total = None
        for k in range(NP):
            term = float(diff[row, k]) * load(k)
            total = term if total is None else total + term
        return total

    lower = lane_masks(FACE)[4]

    def rows_of(k):
        return pl.ds(k * FACE, FACE)

    last = steps - 1
    bottom = plane(lambda k: basis_ref[last, rows_of(k), wide_tile], 0)
    top = plane(lambda k: basis_ref[last, rows_of(k), high_tile], NP - 1)
    message_ref[:FACE] = jnp.where(lower, bottom, top)
    message_ref[FACE:] = jnp.sum(dots_ref[...], axis=1)
    for m in range(steps - 1):
        below = plane(lambda k: ghost[m, rows_of(k), wide_tile], NP - 1)
        above = plane(lambda k: ghost[m, rows_of(k), high_tile], 0)
        near_ref[m] = jnp.where(lower, above, below)


def solve_coefficients(sums):
    size = ITERS
    gram = {}
    for j in range(size):
        for i in range(j + 1):
            at = j * (j + 1) // 2 + i
            gram[j, i] = sums[at : at + 1]
    at = size * (size + 1) // 2
    right = [sums[at + i : at + i + 1] for i in range(size)]
    lower, recip = {}, []
    reduced = {}
    for k in range(size):
        for i in range(k, size):
            value = gram[i, k]
            for m in range(k):
                value = value - lower[i, m] * reduced[k, m]
            reduced[i, k] = value
        pivot = reduced[k, k]
        usable = pivot > 1e-7 * gram[k, k]
        inverse = jnp.where(usable, 1.0 / jnp.where(usable, pivot, 1.0), 0.0)
        recip.append(inverse)
        for i in range(k + 1, size):
            lower[i, k] = reduced[i, k] * inverse
    for k in range(size):
        for m in range(k):
            right[k] = right[k] - lower[k, m] * right[m]
    out = [None] * size
    for k in reversed(range(size)):
        value = right[k] * recip[k]
        for m in range(k + 1, size):
            value = value - lower[m, k] * out[m]
        out[k] = value
    return out


def gradient_kernel(
    diff, sum_a_ref, sum_b_ref, basis_ref, near_ref, fa_ref, fb_ref, dcol_ref,
    *rest,
):
    *grad_refs, vel_ref, work = rest
    elems = basis_ref.shape[2]
    quarter = grad_refs[0].shape[1]
    group = lax.axis_index("grp")
    scalars = jnp.sum(sum_a_ref[...] + sum_b_ref[...], axis=1, keepdims=True)
    part = lax.axis_index("dom")
    parts = lax.axis_size("dom")
    weights = solve_coefficients(scalars)
    tiles = range(elems // TILE)

    @pl.loop(0, NP)
    def _(k):
        rows = pl.ds(pl.multiple_of(k * FACE, FACE), FACE)
        total = weights[0] * basis_ref[0, rows, :]
        for m in range(1, ITERS):
            total = total + weights[m] * basis_ref[m, rows, :]
        vel_ref[rows, :] = total

    lower = lane_masks(FACE)[4]
    x_keep, x_back, y_keep, y_back, _ = lane_masks(FACE)
    odd_part = lax.axis_index("dom") % 2 > 0
    from_above = jnp.where(odd_part, fb_ref[:FACE], fa_ref[:FACE])
    from_below = jnp.where(odd_part, fa_ref[:FACE], fb_ref[:FACE])
    near = weights[ITERS - 1] * jnp.where(lower, from_above, from_below)
    for m in range(ITERS - 1):
        near = near + weights[m] * near_ref[m]
    near = pltpu.roll(near, LAYER, 1)

    def finish(direction, scale):
        share_xy(work, tiles, 0.5)
        if direction == 2:
            first = pl.ds(0, FACE)
            last = pl.ds((NP - 1) * FACE, FACE)
            lows = [work[t, first, :] for t in tiles]
            highs = [work[t, last, :] for t in tiles]
            low_roll = [pltpu.roll(v, LAYER, 1) for v in lows] + [near]
            high_roll = [near] + [pltpu.roll(v, LAYER, 1) for v in highs]
            count = len(tiles)
            for n in tiles:
                up = jnp.where(lower, low_roll[n], low_roll[n + 1])
                down = jnp.where(lower, high_roll[n], high_roll[n + 1])
                high_mean = 0.5 * (highs[n] + up)
                low_mean = 0.5 * (lows[n] + down)
                if n == count - 1:
                    edge = jnp.logical_and(jnp.logical_not(lower), part == parts - 1)
                    high_mean = jnp.where(edge, highs[n], high_mean)
                if n == 0:
                    edge = jnp.logical_and(lower, part == 0)
                    low_mean = jnp.where(edge, lows[n], low_mean)
                work[n, last, :] = high_mean
                work[n, first, :] = low_mean
        for turn, grad_ref in enumerate(grad_refs):
            start = pl.multiple_of(jnp.bitwise_xor(group, turn) * quarter, quarter)
            value = load_block(work, 0, pl.ds(start, quarter)) * scale
            grad_ref[direction] = value.astype(BF16)

    @pl.loop(0, NP)
    def _(k):
        rows = pl.ds(pl.multiple_of(k * FACE, FACE), FACE)
        value = vel_ref[rows, :].reshape(NP, NP, elems)
        total = wide(dcol_ref[0], elems)[None] * value
        for shift in range(1, NP):
            total = total + wide(dcol_ref[shift], elems)[None] * pltpu.roll(value, NP - shift, 1)
        save_block(work, 0, rows, total.reshape(FACE, elems))

    finish(0, 1.0 / NP)

    @pl.loop(0, NP)
    def _(k):
        rows = pl.ds(pl.multiple_of(k * FACE, FACE), FACE)
        value = vel_ref[rows, :].reshape(NP, NP, elems)
        for j in range(NP):
            total = float(diff[j, 0]) * value[0]
            for m in range(1, NP):
                total = total + float(diff[j, m]) * value[m]
            save_block(work, 0, pl.ds(pl.multiple_of(k * FACE + j * NP, NP), NP), total)

    finish(1, 1.0 / NP)

    @pl.loop(0, NP)
    def _(j):
        planes = [vel_ref[pl.ds(pl.multiple_of(m * FACE + j * NP, NP), NP), :] for m in range(NP)]
        for k in range(NP):
            total = float(diff[k, 0]) * planes[0]
            for m in range(1, NP):
                total = total + float(diff[k, m]) * planes[m]
            save_block(work, 0, pl.ds(pl.multiple_of(k * FACE + j * NP, NP), NP), total)

    finish(2, 1.0 / NP)


def slots_kernel(order_ref, vel_ref, out_ref):
    elems = order_ref.shape[1]
    cell_by_slot = (iota((elems, elems), 0) == order_ref[...]).astype(F32)
    pick = jnp.transpose(cell_by_slot).astype(BF16)
    high, mid, low = split3(vel_ref[...])
    out_ref[...] = dot_nt(pick, high) + dot_nt(pick, mid) + dot_nt(pick, low)


def middle_eigenvalue(jac):
    strain = [[0.5 * (jac[a][b] + jac[b][a]) for b in range(3)] for a in range(3)]
    spin = [[0.5 * (jac[a][b] - jac[b][a]) for b in range(3)] for a in range(3)]
    mat = [[None] * 3 for _ in range(3)]
    for a in range(3):
        for b in range(a, 3):
            total = strain[a][0] * strain[0][b] + spin[a][0] * spin[0][b]
            for c in (1, 2):
                total = total + strain[a][c] * strain[c][b] + spin[a][c] * spin[c][b]
            mat[a][b] = total
            mat[b][a] = total
    peak = jnp.maximum(jnp.abs(mat[0][1]), jnp.maximum(jnp.abs(mat[0][2]), jnp.abs(mat[1][2])))
    for a in range(3):
        peak = jnp.maximum(peak, jnp.abs(mat[a][a]))
    peak = jnp.where(peak > 0.0, peak, 1.0)
    shrink = 1.0 / peak
    for a in range(3):
        for b in range(a, 3):
            mat[a][b] = mat[b][a] = mat[a][b] * shrink
    for _ in range(SWEEPS):
        for p, q, r in ((0, 1, 2), (0, 2, 1), (1, 2, 0)):
            pivot = mat[p][q]
            first, second = mat[p][p], mat[q][q]
            gap = 0.5 * (first - second)
            norm = pivot * pivot + gap * gap
            inv_norm = lax.rsqrt(jnp.maximum(norm, 1e-37))
            middle = 0.5 * (first + second)
            radius = norm * inv_norm
            turned = norm > 0.0
            cos_two = jnp.where(turned, gap * inv_norm, 1.0)
            half_sin = (0.5 * pivot) * inv_norm
            lead = 0.5 + 0.5 * jnp.abs(cos_two)
            inv_big = lax.rsqrt(lead)
            big = lead * inv_big
            small = half_sin * inv_big
            forward = cos_two >= 0.0
            cosine = jnp.where(forward, big, jnp.abs(small))
            sine = jnp.where(forward, small, jnp.where(pivot < 0.0, -big, big))
            mat[p][p] = middle + radius
            mat[q][q] = middle - radius
            mat[p][q] = mat[q][p] = None
            side_p, side_q = mat[r][p], mat[r][q]
            if side_p is None:
                new_p, new_q = sine * side_q, cosine * side_q
            elif side_q is None:
                new_p, new_q = cosine * side_p, -(sine * side_p)
            else:
                new_p = cosine * side_p + sine * side_q
                new_q = cosine * side_q - sine * side_p
            mat[r][p] = mat[p][r] = new_p
            mat[r][q] = mat[q][r] = new_q
    d0, d1, d2 = mat[0][0], mat[1][1], mat[2][2]
    largest = jnp.maximum(jnp.maximum(d0, d1), d2)
    smallest = jnp.minimum(jnp.minimum(d0, d1), d2)
    return (d0 + d1 + d2 - largest - smallest) * peak


def vortex_kernel(*refs):
    *grad_refs, place_ref, out_ref, value = refs
    rows_all = grad_refs[0].shape[1]
    group = lax.axis_index("grp")

    def component(c, d, rows):
        turn = jnp.bitwise_xor(group, c)
        out = grad_refs[-1][d, rows, :].astype(F32)
        for n in reversed(range(len(grad_refs) - 1)):
            out = jnp.where(turn == n, grad_refs[n][d, rows, :].astype(F32), out)
        return out

    step = 16

    @pl.loop(0, rows_all // step)
    def _(n):
        rows = pl.ds(pl.multiple_of(n * step, step), step)
        jac = [[component(c, d, rows) for d in range(3)] for c in range(3)]
        value[rows, :] = middle_eigenvalue(jac)

    high, mid, low = split3(value[...])
    place = place_ref[...]
    moved = dot_nt(place, high) + dot_nt(place, mid) + dot_nt(place, low)
    out_ref[...] = moved.reshape(out_ref.shape)


def final_kernel(*refs):
    *vortex_refs, vel_ref, out_ref = refs
    quarters = len(vortex_refs)
    quarter = vortex_refs[0].shape[1]

    last = lax.axis_index("grp") == lax.axis_size("grp") - 1

    @pl.when(last)
    def _():
        for q in range(quarters):
            out_ref[0, :, q * quarter : (q + 1) * quarter] = vortex_refs[(quarters - 1) ^ q][...]

    @pl.when(jnp.logical_not(last))
    def _():
        out_ref[0] = vel_ref[...]


PREP_LIMIT = 67043328 - 2600 * 1024
GRANT = pltpu.CompilerParams(vmem_limit_bytes=24 * 2**20)


def vmem():
    return pl.BlockSpec(memory_space=pltpu.VMEM)


def cost(flops, size):
    return pl.CostEstimate(flops=flops, bytes_accessed=size, transcendentals=0)


def per_device(forcing, viscosity, mass_coef, element_order, owner):
    elems = viscosity.shape[0]
    nodes = forcing.shape[2]
    parts = lax.axis_size("dom")
    groups = lax.axis_size("grp")
    cap = elems // parts
    quarter = nodes // groups
    diff, kmat_np, cols_np, dcol_np, bound = host_tables()
    kmat = jnp.asarray(kmat_np, BF16)
    cols = jnp.asarray(cols_np)
    dcol = jnp.asarray(dcol_np)
    sds = jax.ShapeDtypeStruct

    pack = pl.pallas_call(
        prep_kernel,
        in_specs=[pl.BlockSpec(memory_space=pltpu.HBM)] * 5,
        out_specs=vmem(),
        out_shape=sds((nodes + 8, elems), F32),
        scratch_shapes=[
            pltpu.VMEM((elems, nodes), F32),
            pltpu.VMEM((1, elems), jnp.int32),
            pltpu.VMEM((1, elems), F32),
            pltpu.VMEM((1, elems), F32),
            pltpu.VMEM((nodes, TILE), F32),
            pltpu.SemaphoreType.DMA((5,)),
        ],
        cost_estimate=cost(10**9, 2 * 10**6),
        compiler_params=pltpu.CompilerParams(vmem_limit_bytes=PREP_LIMIT),
        name="prep",
    )(forcing, element_order, viscosity[None], mass_coef[None], cols)

    swap_a = [(i, i ^ 1) for i in range(parts) if i ^ 1 < parts]
    swap_b = [(i, ((i - 1) ^ 1) + 1) for i in range(1, parts - 1)]
    ghost_b = lax.ppermute(pack, "dom", swap_b)
    ghost_a = lax.ppermute(pack, "dom", swap_a)

    raw, rhs_xy, jac_xy = pl.pallas_call(
        stage_kernel,
        in_specs=[vmem()] * 2,
        out_specs=[vmem()] * 3,
        out_shape=[
            sds((nodes + 8, elems), F32),
            sds((2, nodes, TILE), F32),
            sds((2, nodes, TILE), F32),
        ],
        cost_estimate=cost(10**9, 2 * 10**6),
        compiler_params=GRANT,
        name="stage",
    )(pack, cols)

    place = pl.pallas_call(
        lambda *refs: place_kernel(cap, *refs),
        in_specs=[vmem(), vmem()],
        out_specs=vmem(),
        out_shape=sds((elems, elems), BF16),
        cost_estimate=cost(10**9, 2 * 10**6),
        compiler_params=GRANT,
        name="place",
    )(element_order, owner)

    basis, near, message = pl.pallas_call(
        lambda *refs: krylov_kernel(diff, bound, *refs),
        in_specs=[vmem()] * 7,
        out_specs=[vmem()] * 3,
        out_shape=[
            sds((ITERS, nodes, elems), F32),
            sds((ITERS - 1, FACE, TILE), F32),
            sds((FACE + 16, TILE), F32),
        ],
        scratch_shapes=[
            pltpu.VMEM((6, nodes, TILE), F32),
            pltpu.VMEM((3, 8, elems), F32),
            pltpu.VMEM((6, nodes, TILE), F32),
            pltpu.VMEM((nodes, elems), F32),
            pltpu.VMEM((ITERS - 1, nodes, elems), F32),
            pltpu.VMEM((2, nodes // 2, elems), BF16),
            pltpu.VMEM((2, nodes // 2, elems), BF16),
            pltpu.VMEM((2, nodes // 2, elems), F32),
            pltpu.VMEM((16, 8, TILE), F32),
        ],
        cost_estimate=cost(10**10, 10**7),
        compiler_params=GRANT,
        name="krylov",
    )(raw, rhs_xy, jac_xy, ghost_a, ghost_b, kmat, cols)

    face_a = lax.ppermute(message, "dom", swap_a)
    face_b = lax.ppermute(message, "dom", swap_b)
    pending = (message[FACE:], face_a[FACE:])
    reach = 2
    while reach < parts:
        sums = pending[0] + pending[1]
        pending = (sums, lax.ppermute(sums, "dom", [(i, i ^ reach) for i in range(parts)]))
        reach *= 2

    *grads, vel = pl.pallas_call(
        lambda *refs: gradient_kernel(diff, *refs),
        in_specs=[vmem()] * 7,
        out_specs=[vmem()] * (groups + 1),
        out_shape=[sds((3, quarter, elems), BF16)] * groups + [sds((nodes, elems), F32)],
        scratch_shapes=[pltpu.VMEM((2, nodes, TILE), F32)],
        cost_estimate=cost(10**9, 4 * 10**6),
        compiler_params=GRANT,
        name="gradient",
    )(*pending, basis, near, face_a, face_b, dcol)

    exchanged = [grads[0]] + [
        lax.ppermute(grads[turn], "grp", [(i, i ^ turn) for i in range(groups)])
        for turn in range(1, groups)
    ]

    vel_slot = pl.pallas_call(
        slots_kernel,
        in_specs=[vmem(), vmem()],
        out_specs=vmem(),
        out_shape=sds((elems, nodes), F32),
        cost_estimate=cost(10**9, 2 * 10**6),
        compiler_params=GRANT,
        name="slots",
    )(element_order, vel)

    packed = pl.pallas_call(
        vortex_kernel,
        in_specs=[vmem()] * (groups + 1),
        out_specs=vmem(),
        out_shape=sds((parts, cap, quarter), F32),
        scratch_shapes=[pltpu.VMEM((quarter, elems), F32)],
        cost_estimate=cost(10**9, 2 * 10**6),
        compiler_params=GRANT,
        name="vortex",
    )(*exchanged, place)

    received = lax.all_to_all(packed, "dom", split_axis=0, concat_axis=0, tiled=True)
    received = received.reshape(elems, quarter)
    gathered = [received] + [
        lax.ppermute(received, "grp", [(i, i ^ turn) for i in range(groups)])
        for turn in range(1, groups)
    ]
    return pl.pallas_call(
        final_kernel,
        in_specs=[vmem()] * (groups + 1),
        out_specs=vmem(),
        out_shape=sds((1, elems, nodes), F32),
        cost_estimate=cost(10**6, 2 * 10**6),
        compiler_params=GRANT,
        name="final",
    )(*gathered, vel_slot)


def solution(mesh):
    in_specs = (P(None, "dom", None), P("dom"), P("dom"), P("dom", None), P("dom", None))
    out_specs = P("grp", "dom", None)
    return jax.shard_map(
        per_device, mesh=mesh, in_specs=in_specs, out_specs=out_specs, check_vma=False
    )
```
